512 devices in a mesh: section: 8 (over z), sht: 64 (over x, y, core).
Axes of the slice: x: 4, y: 8, z: 8, core: 2. Of those that a mesh axis runs over, the one named last changes fastest.
Arguments:
- analysis: bfloat16 [128, 256, 192], P('sht', None, 'section'), may hold values from -6 to 6
- perturbations: bfloat16 [6, 128, 256, 192], P(None, 'sht', None, 'section'), may hold values from -6 to 6
- gain_first: float32 [8, 192], P('section'), may hold values from 0.1 to 1.9
- spectral_gain: float32 [8, 2, 24576], P('section'), may hold values from -6 to 6
- skip_weight: bfloat16 [8, 192, 192], P('section'), may hold values from -0.4375 to 0.4375
- gain_second: float32 [8, 192], P('section'), may hold values from 0.1 to 1.9
- mlp_in: bfloat16 [8, 192, 384], P('section'), may hold values from -0.4375 to 0.4375
- mlp_out: bfloat16 [8, 192, 384], P('section'), may hold values from -0.3125 to 0.3125
Outputs:
- block_outputs: bfloat16 [8, 6, 128, 49152], P('section', None, 'sht')
The draws below stay inside these ranges and needn't reach their ends.
All inputs are finite; a program needn't handle non-finite values.
Results may differ from the reference program's by a relative error of at most 0.025.
Values may be sent and summed in bfloat16 or wider, within the bound.
A program may use at most 64 MiB of HBM per device.

```python
import math
import jax
import jax.numpy as jnp
from jax import lax

C = 192
HID = 384
NLAT = 128
NLON = 256
LMAX = 128
MMAX = 128
MEMBERS = 6
BLOCKS = 8
N_SECTION = 8


def level_of(stream_key, dims, shards, low, largest):
    def one(position, blocks):
        draws = jax.random.uniform(jax.random.fold_in(jax.random.fold_in(stream_key, 6), position), (blocks,), jnp.float32, low / len(shards), largest / len(shards))
        return jnp.repeat(jnp.exp(draws), dims[position] // blocks).reshape((-1,) + (1,) * (len(dims) - position - 1))

    gain = one(*shards[0])
    for cut in shards[1:]:
        gain = gain * one(*cut)
    return gain


def noise(own_key, shape, spread, most, cuts=(), held_as=jnp.bfloat16):
    result = jax.random.normal(own_key, shape, jnp.float32) * spread
    if len(cuts) > 0:
        result = level_of(own_key, shape, cuts, -0.22, 0.18) * result
    return jnp.clip(result, min=-most, max=most).astype(held_as)


def setup_inputs(seed: int = 0) -> dict:
    keys = jax.random.split(jax.random.key(seed), 9)
    return {
        "analysis": noise(keys[0], (NLAT, NLON, C), 1.0, 6.0, ((0, 64), (2, 8))),
        "perturbations": noise(keys[1], (MEMBERS, NLAT, NLON, C), 1.0, 6.0, ((1, 64), (3, 8))),
        "gain_first": jnp.clip(1.0 + 0.18 * jax.random.normal(keys[2], (BLOCKS, C), jnp.float32), 0.1, 1.9),
        "spectral_gain": noise(keys[3], (BLOCKS, 2, LMAX * C), 1.0, 6.0, ((0, 8),), jnp.float32),
        "skip_weight": noise(keys[4], (BLOCKS, C, C), C ** -0.5, 0.4375, ((0, 8),)),
        "gain_second": jnp.clip(1.0 + 0.18 * jax.random.normal(keys[5], (BLOCKS, C), jnp.float32), 0.1, 1.9),
        "mlp_in": noise(keys[6], (BLOCKS, C, HID), C ** -0.5, 0.4375, ((0, 8),)),
        "mlp_out": noise(keys[7], (BLOCKS, C, HID), HID ** -0.5, 0.3125, ((0, 8),)),
    }


def legendre_table(nlat, lmax, mmax, nlon, m_first, m_count):
    latitudes = jnp.arange(nlat, dtype=jnp.float32)
    colatitude = math.pi * (latitudes + 0.5) / nlat
    cosine = jnp.cos(colatitude)
    sine = jnp.sin(colatitude)
    orders = jnp.arange(1, mmax, dtype=jnp.float32)
    factors = jnp.cumsum(0.5 * jnp.log((2.0 * orders + 1.0) / (2.0 * orders)))
    log_diag = jnp.concatenate([jnp.zeros((1,), jnp.float32), factors])
    m_index = m_first + jnp.arange(m_count, dtype=jnp.int32)
    picked = lax.optimization_barrier(jnp.sum(jnp.where(m_index[:, None] == jnp.arange(mmax, dtype=jnp.int32)[None, :], log_diag[None, :], 0.0), axis=1))
    m_float = m_index.astype(jnp.float32)
    diagonal = jnp.exp(picked[None, :] + m_float[None, :] * jnp.log(sine)[:, None]) * math.sqrt(0.25 / math.pi)
    cos_col = cosine[:, None]

    def advance(carry, degree):
        latest, earlier = carry
        degree_float = degree.astype(jnp.float32)
        lower = jnp.sqrt((4.0 * degree_float * degree_float - 1.0) / jnp.maximum(degree_float * degree_float - m_float * m_float, 1.0))
        shifted = degree_float - 1.0
        upper = jnp.sqrt(jnp.maximum(shifted * shifted - m_float * m_float, 0.0) / jnp.maximum(4.0 * shifted * shifted - 1.0, 1.0))
        recurred = lower[None, :] * (cos_col * latest - upper[None, :] * earlier)
        first_step = jnp.sqrt(2.0 * m_float + 3.0)[None, :] * cos_col * diagonal
        current = jnp.where(degree == m_index[None, :], diagonal, jnp.where(degree == m_index[None, :] + 1, first_step, jnp.where(degree > m_index[None, :] + 1, recurred, 0.0)))
        return ((current, latest), current)
    initial = jnp.zeros((nlat, m_count), jnp.float32)
    _, stacked = lax.scan(advance, (initial, initial), jnp.arange(lmax, dtype=jnp.int32), unroll=8)
    legendre = jnp.transpose(stacked, (1, 0, 2))
    weights = sine * (2.0 * math.pi / nlon) * (math.pi / nlat)
    return (legendre, weights)

def fourier_tables(nlon, mmax):
    samples = jnp.arange(nlon, dtype=jnp.int32)
    orders = jnp.arange(mmax, dtype=jnp.int32)
    phase = (samples[:, None] * orders[None, :] % nlon).astype(jnp.float32) * (2.0 * math.pi / nlon)
    cosines = jnp.cos(phase)
    sines = jnp.sin(phase)
    forward = jnp.stack([cosines, -sines], axis=1).astype(jnp.bfloat16)
    factor = jnp.where(orders == 0, 1.0, 2.0).astype(jnp.float32)
    inverse = jnp.stack([cosines.T * factor[:, None], -sines.T * factor[:, None]], axis=0).astype(jnp.bfloat16)
    return (forward, inverse)

def layer_norm(values, gain_vector):
    average = lax.optimization_barrier(jnp.mean(values, axis=-1, keepdims=True))
    centred = values - average
    variance = lax.optimization_barrier(jnp.mean(centred * centred, axis=-1, keepdims=True))
    return centred * lax.rsqrt(variance + 1e-05) * gain_vector

def apply_gain(coeffs, gain_table):
    real_part = coeffs[:, :, :, 0]
    imag_part = coeffs[:, :, :, 1]
    gain_real = gain_table[0][None, :, None, :]
    gain_imag = gain_table[1][None, :, None, :]
    return jnp.stack([real_part * gain_real - imag_part * gain_imag, real_part * gain_imag + imag_part * gain_real], axis=3)

def project_out(hidden, out_matrix):
    return lax.dot_general(hidden, out_matrix, (((1,), (1,)), ((), ())), preferred_element_type=jnp.float32)

def sfno_block(current_state, gain_one, gain_flat, skip_matrix, gain_two, first_matrix, second_matrix, weighted, plain_table, forward, inverse):
    state_wide = current_state.astype(jnp.float32)
    channels = current_state.shape[-1]
    gain_table = gain_flat.reshape(2, -1, channels)
    normed = layer_norm(state_wide, gain_one).astype(jnp.bfloat16)
    spectrum = jnp.einsum('bjkc,kpm->bjmpc', normed.astype(jnp.float32), forward.astype(jnp.float32)).astype(jnp.bfloat16)
    coeffs = jnp.einsum('jlm,bjmpc->blmpc', weighted.astype(jnp.float32), spectrum.astype(jnp.float32))
    filtered = apply_gain(coeffs, gain_table).astype(jnp.bfloat16)
    returned = jnp.einsum('jlm,blmpc->bjmpc', plain_table.astype(jnp.float32), filtered.astype(jnp.float32)).astype(jnp.bfloat16)
    spatial = jnp.einsum('bjmpc,pmk->bjkc', returned.astype(jnp.float32), inverse.astype(jnp.float32))
    skipped = jnp.dot(normed.reshape(-1, channels), skip_matrix, preferred_element_type=jnp.float32).reshape(spatial.shape)
    activated = jax.nn.gelu(spatial + skipped, approximate=False)
    second = layer_norm(activated, gain_two).astype(jnp.bfloat16)
    hidden = jax.nn.gelu(jnp.dot(second.reshape(-1, channels), first_matrix, preferred_element_type=jnp.float32), approximate=False).astype(jnp.bfloat16)
    update = project_out(hidden, second_matrix).reshape(spatial.shape)
    return (state_wide + update).astype(jnp.bfloat16)

def reference(analysis, perturbations, gain_first, spectral_gain, skip_weight, gain_second, mlp_in, mlp_out):
    legendre, weights = legendre_table(NLAT, LMAX, MMAX, NLON, 0, MMAX)
    weighted = (legendre * weights[:, None, None]).astype(jnp.bfloat16)
    plain_table = legendre.astype(jnp.bfloat16)
    forward, inverse = fourier_tables(NLON, MMAX)
    pert_wide = perturbations.astype(jnp.float32)
    current_state = (analysis.astype(jnp.float32)[None] + pert_wide - lax.optimization_barrier(jnp.mean(pert_wide, axis=0, keepdims=True))).astype(jnp.bfloat16)
    outputs = []
    for block_index in range(N_SECTION):
        current_state = sfno_block(current_state, gain_first[block_index], spectral_gain[block_index], skip_weight[block_index], gain_second[block_index], mlp_in[block_index], mlp_out[block_index], weighted, plain_table, forward, inverse)
        outputs.append(current_state.reshape(MEMBERS, NLAT, NLON * C))
    return jnp.stack(outputs)
```

```python
import math

import jax
import jax.numpy as jnp
from jax import lax
from jax.experimental import pallas as pl
from jax.sharding import PartitionSpec as P

C = 192
NLAT = 128
NLON = 256
LMAX = 128
MMAX = 128


def recurrence_kernel(lower_ref, upper_ref, first_ref, cosine_ref, diagonal_ref, table_ref):
    cosine = cosine_ref[...]
    diagonal = diagonal_ref[...]

    def advance(degree, carry):
        latest, earlier = carry
        current = (
            lower_ref[degree] * (cosine * latest - upper_ref[degree] * earlier)
            + first_ref[degree] * diagonal
        )
        table_ref[degree] = current
        return (current, latest)

    initial = cosine * 0.0
    lax.fori_loop(0, LMAX, advance, (initial, initial), unroll=8)


def legendre_table(m_first, m_count):
    latitudes = jnp.arange(NLAT, dtype=jnp.float32)
    colatitude = math.pi * (latitudes + 0.5) / NLAT
    cosine = jnp.cos(colatitude)
    sine = jnp.sin(colatitude)
    orders = jnp.arange(1, MMAX, dtype=jnp.float32)
    factors = jnp.cumsum(0.5 * jnp.log((2.0 * orders + 1.0) / (2.0 * orders)))
    log_diag = jnp.concatenate([jnp.zeros((1,), jnp.float32), factors])
    m_index = m_first + jnp.arange(m_count, dtype=jnp.int32)
    picked = jnp.sum(
        jnp.where(
            m_index[:, None] == jnp.arange(MMAX, dtype=jnp.int32)[None, :], log_diag[None, :], 0.0
        ),
        axis=1,
    )
    m_float = m_index.astype(jnp.float32)
    diagonal = jnp.exp(picked[:, None] + m_float[:, None] * jnp.log(sine)[None, :]) * math.sqrt(
        0.25 / math.pi
    )
    degree = jnp.arange(LMAX, dtype=jnp.float32)[:, None]
    order = m_float[None, :]
    lower = jnp.sqrt(
        jnp.maximum(4.0 * degree * degree - 1.0, 0.0)
        / jnp.maximum(degree * degree - order * order, 1.0)
    )
    shifted = degree - 1.0
    upper = jnp.sqrt(
        jnp.maximum(shifted * shifted - order * order, 0.0)
        / jnp.maximum(4.0 * shifted * shifted - 1.0, 1.0)
    )
    first = jnp.where(degree == order, 1.0, 0.0)
    wide = lambda x: jnp.broadcast_to(x[:, :, None], (LMAX, m_count, NLAT))
    table = pl.pallas_call(
        recurrence_kernel,
        out_shape=jax.ShapeDtypeStruct((LMAX, m_count, NLAT), jnp.float32),
    )(
        wide(lower),
        wide(upper),
        wide(first),
        jnp.broadcast_to(cosine[None, :], (m_count, NLAT)),
        diagonal,
    )
    weights = sine * (2.0 * math.pi / NLON) * (math.pi / NLAT)
    return (table, weights)


def fourier_tables(nlon, mmax):
    samples = jnp.arange(nlon, dtype=jnp.int32)
    orders = jnp.arange(mmax, dtype=jnp.int32)
    phase = (samples[:, None] * orders[None, :] % nlon).astype(jnp.float32) * (2.0 * math.pi / nlon)
    cosines = jnp.cos(phase)
    sines = jnp.sin(phase)
    forward = jnp.stack([cosines, -sines], axis=1).astype(jnp.bfloat16)
    factor = jnp.where(orders == 0, 1.0, 2.0).astype(jnp.float32)
    inverse = jnp.stack([cosines.T * factor[:, None], -sines.T * factor[:, None]], axis=0).astype(
        jnp.bfloat16
    )
    return (forward, inverse)


def layer_norm(values, gain_vector):
    average = jnp.mean(values, axis=-1, keepdims=True)
    centred = values - average
    variance = jnp.mean(centred * centred, axis=-1, keepdims=True)
    return centred * lax.rsqrt(variance + 1e-05) * gain_vector


def apply_gain(coeffs, gain_table):
    real_part = coeffs[:, :, :, 0]
    imag_part = coeffs[:, :, :, 1]
    gain_real = gain_table[0][None, :, None, :]
    gain_imag = gain_table[1][None, :, None, :]
    return jnp.stack(
        [
            real_part * gain_real - imag_part * gain_imag,
            real_part * gain_imag + imag_part * gain_real,
        ],
        axis=3,
    )


def recenter(analysis, perturbations):
    pert_wide = perturbations.astype(jnp.float32)
    average = jnp.mean(pert_wide, axis=0, keepdims=True)
    return (analysis.astype(jnp.float32)[None] + pert_wide - average).astype(jnp.bfloat16)


def per_device(
    analysis, perturbations, gain_first, spectral_gain, skip_weight, gain_second, mlp_in, mlp_out
):
    count = lax.axis_size("section")
    member_count = perturbations.shape[0]
    m_count = MMAX // lax.axis_size("sht")
    members = recenter(analysis, perturbations)
    members = jnp.pad(members, ((0, count - member_count), (0, 0), (0, 0), (0, 0)))
    slices = lax.all_to_all(members, "section", split_axis=0, concat_axis=0, tiled=True)
    state = jnp.moveaxis(slices, 0, 2).reshape(1, slices.shape[1], NLON, C)
    gains = lax.all_gather(jnp.concatenate([gain_first, gain_second], axis=0), "section")
    filters = lax.all_gather(spectral_gain[0].astype(jnp.bfloat16), "section")
    matrices = lax.all_gather(
        jnp.concatenate([skip_weight[0], mlp_in[0], mlp_out[0]], axis=1), "section"
    )
    pick = lambda stack, block: lax.dynamic_index_in_dim(stack, block, 0, keepdims=False)
    forward, inverse = fourier_tables(NLON, MMAX)
    legendre, weights = legendre_table(lax.axis_index("sht") * m_count, m_count)
    weighted = (legendre * weights[None, None, :]).astype(jnp.bfloat16)
    plain_table = legendre.astype(jnp.bfloat16)

    def spectral(normed, full_gain):
        batch_rows = normed.shape[0]
        lat_rows = normed.shape[1]
        spectrum = jnp.einsum(
            "bjkc,kpm->bjmpc", normed, forward, preferred_element_type=jnp.float32
        ).astype(jnp.bfloat16)
        spectrum = spectrum.reshape(batch_rows, lat_rows, MMAX, 2 * C)
        exchanged = lax.all_to_all(spectrum, "sht", split_axis=2, concat_axis=1, tiled=True)
        item_count = exchanged.shape[0]
        coeffs = jnp.einsum(
            "lmj,bjmq->blmq", weighted, exchanged, preferred_element_type=jnp.float32
        )
        coeffs = coeffs.reshape(item_count, LMAX, m_count, 2, C)
        filtered = (
            apply_gain(coeffs, full_gain)
            .astype(jnp.bfloat16)
            .reshape(item_count, LMAX, m_count, 2 * C)
        )
        returned = jnp.einsum(
            "lmj,blmq->bjmq", plain_table, filtered, preferred_element_type=jnp.float32
        ).astype(jnp.bfloat16)
        returned = lax.all_to_all(returned, "sht", split_axis=1, concat_axis=2, tiled=True)
        returned = returned.reshape(batch_rows, lat_rows, MMAX, 2, C)
        return jnp.einsum("bjmpc,pmk->bjkc", returned, inverse, preferred_element_type=jnp.float32)

    def step(block, carry):
        state, stored = carry
        block_matrices = pick(matrices, block)
        block_gains = pick(gains, block)
        full_gain = pick(filters, block).reshape(2, LMAX, C).astype(jnp.float32)
        skip = block_matrices[:, :C]
        first_matrix = block_matrices[:, C : 3 * C]
        second_matrix = block_matrices[:, 3 * C :]
        state_wide = state.astype(jnp.float32)
        normed = layer_norm(state_wide, block_gains[0]).astype(jnp.bfloat16)
        spatial = spectral(normed, full_gain)
        skipped = jnp.dot(
            normed.reshape(-1, C), skip, preferred_element_type=jnp.float32
        ).reshape(spatial.shape)
        activated = jax.nn.gelu(spatial + skipped, approximate=False)
        second = layer_norm(activated, block_gains[1]).astype(jnp.bfloat16)
        hidden = jax.nn.gelu(
            jnp.dot(second.reshape(-1, C), first_matrix, preferred_element_type=jnp.float32),
            approximate=False,
        ).astype(jnp.bfloat16)
        update = lax.dot_general(
            hidden, second_matrix, (((1,), (1,)), ((), ())), preferred_element_type=jnp.float32
        ).reshape(spatial.shape)
        state = (state_wide + update).astype(jnp.bfloat16)
        return (state, lax.dynamic_update_slice_in_dim(stored, state, block, 0))

    empty = jnp.zeros((count, *state.shape[1:]), jnp.bfloat16)
    _, stacked = lax.fori_loop(0, count, step, (state, empty))
    stored = lax.all_to_all(stacked, "section", split_axis=0, concat_axis=0, tiled=True)
    stored = stored[:member_count]
    return stored.reshape(1, member_count, stored.shape[1], NLON * C)


def solution(mesh):
    return jax.shard_map(
        per_device,
        mesh=mesh,
        in_specs=(
            P("sht", None, "section"),
            P(None, "sht", None, "section"),
            P("section", None),
            P("section", None, None),
            P("section", None, None),
            P("section", None),
            P("section", None, None),
            P("section", None, None),
        ),
        out_specs=P("section", None, "sht", None),
        check_vma=False,
    )
```

```python
import math

import jax
import jax.numpy as jnp
import numpy as np
from jax import lax
from jax.experimental import pallas as pl
from jax.experimental.pallas import tpu as pltpu
from jax.sharding import PartitionSpec as P

C = 192
HID = 384
NLAT = 128
NLON = 256
LMAX = 128
MMAX = 128
MEMBERS = 6
SECTIONS = 8
SHT = 64
IDLE = 2
PAD = 256
HALF = 128
MESH = pl.DeviceIdType.MESH
BF = jnp.bfloat16
F32 = jnp.float32


def longitude_tables():
    order = np.concatenate([np.arange(0, NLON, 2), np.arange(1, NLON, 2)])
    waves = np.arange(MMAX)
    phase = (waves[:, None] * order[None, :] % NLON).astype(np.float32) * np.float32(
        2.0 * math.pi / NLON
    )
    cosines = np.cos(phase)
    sines = np.sin(phase)
    forward = np.stack([cosines, -sines])
    factor = np.where(waves == 0, 1.0, 2.0).astype(np.float32)
    inverse = np.concatenate([cosines.T * factor, -sines.T * factor], axis=1)
    return jnp.asarray(forward, BF), jnp.asarray(inverse, BF)


def latitude_rows():
    lane = np.arange(2 * NLAT)
    colatitude = (math.pi * (lane // 2 + 0.5) / NLAT).astype(np.float32)
    sine = np.sin(colatitude)
    rows = np.zeros((8, 2 * NLAT), np.float32)
    rows[0] = np.cos(colatitude)
    rows[1] = sine
    rows[2] = np.log(sine)
    rows[3] = sine * (2.0 * math.pi / NLON) * (math.pi / NLAT)
    rows[4] = lane % 2
    return jnp.asarray(rows)


def gelu(x):
    return 0.5 * x * (1.0 + lax.erf(x * math.sqrt(0.5)))


def lane_of(shape):
    return lax.broadcasted_iota(jnp.int32, shape, len(shape) - 1)


def layer_norm(values, gain_row):
    average = jnp.sum(values, axis=1, keepdims=True) * (1.0 / C)
    centred = jnp.where(lane_of(values.shape) < C, values - average, 0.0)
    variance = jnp.sum(centred * centred, axis=1, keepdims=True) * (1.0 / C)
    return centred * lax.rsqrt(variance + 1e-05) * gain_row


def dot(a, b):
    return jnp.dot(a, b, preferred_element_type=F32)


def build_legendre(me, rows_ref, lower, upper, first, table, forward_table, inverse_table):
    cosine = rows_ref[0:1, :]
    parity = rows_ref[4:5, :]
    order = parity + (2 * me).astype(F32)
    shape = (LMAX, 2 * NLAT)
    degree = lax.broadcasted_iota(jnp.int32, shape, 0).astype(F32)
    step = degree + 1.0
    terms = jnp.where(step <= order, 0.5 * jnp.log((2.0 * step + 1.0) / (2.0 * step)), 0.0)
    picked = jnp.sum(terms, axis=0, keepdims=True)
    diagonal = jnp.exp(picked + order * rows_ref[2:3, :]) * math.sqrt(0.25 / math.pi)
    lower[...] = jnp.sqrt(
        jnp.maximum(4.0 * degree * degree - 1.0, 0.0)
        / jnp.maximum(degree * degree - order * order, 1.0)
    )
    shifted = degree - 1.0
    upper[...] = jnp.sqrt(
        jnp.maximum(shifted * shifted - order * order, 0.0)
        / jnp.maximum(4.0 * shifted * shifted - 1.0, 1.0)
    )
    first[...] = jnp.where(degree == order, diagonal, 0.0)

    def advance(row, carry):
        latest, earlier = carry
        at = pl.ds(row, 1)
        current = lower[at, :] * (cosine * latest - upper[at, :] * earlier) + first[at, :]
        table[at, :] = current
        return (current, latest)

    zero = cosine * 0.0
    lax.fori_loop(0, LMAX, advance, (zero, zero), unroll=8)
    plain = table[...]
    weighted = plain * rows_ref[3:4, :]
    even = jnp.broadcast_to(parity, shape) < 0.5
    forward_table[0:LMAX, :] = jnp.where(even, weighted, 0.0).astype(BF)
    forward_table[LMAX:, :] = jnp.where(even, 0.0, weighted).astype(BF)
    inverse_table[:, 0:LMAX] = jnp.where(even, plain, 0.0).T.astype(BF)
    inverse_table[:, LMAX:] = jnp.where(even, 0.0, plain).T.astype(BF)


def kernel(
    state_in, gains_in, filter_in, matrix_in, fourier, inverse_fourier, rows,
    out,
    state, normed, skipped, send_one, send_two, recv_one, recv_two,
    gains, filters, matrices, lower, upper, first, table, legendre, legendre_back, leaving,
    sent_one, sent_two, got_one, got_two, weight_sent, weight_got,
    share_sent, share_got, out_sent, out_got, pace,
):
    section = lax.axis_index("section")
    me = lax.axis_index("sht")
    core = lax.rem(me, 2)
    sibling = me + 1 - 2 * core

    barrier = pltpu.get_barrier_semaphore()

    def greet(t, carry):
        pl.semaphore_signal(
            barrier, inc=1, device_id={"sht": lax.rem(me + t, SHT)}, device_id_type=MESH
        )
        return carry

    def greet_column(t, carry):
        pl.semaphore_signal(
            barrier, inc=1, device_id={"section": lax.rem(section + t, SECTIONS)},
            device_id_type=MESH,
        )
        return carry

    lax.fori_loop(1, SHT, greet, 0)
    lax.fori_loop(1, SECTIONS, greet_column, 0)

    matrices[:, C:, :] = jnp.zeros((SECTIONS, PAD - C, 1024), BF)
    matrices[section, 0:C, :] = matrix_in[...]
    filters[section] = filter_in[...]
    gains[section] = gains_in[...]
    build_legendre(me, rows, lower, upper, first, table, legendre, legendre_back)
    state[...] = state_in[...]

    pl.semaphore_wait(barrier, SHT - 1 + SECTIONS - 1)

    filter_half = pl.ds(pl.multiple_of(core * (LMAX // 2), LMAX // 2), LMAX // 2)
    matrix_half = pl.ds(pl.multiple_of(core * (C // 2), C // 2), C // 2)

    def weight_copies(target):
        refs = [
            (gains_in, gains.at[section]),
            (filter_in.at[filter_half], filters.at[section, filter_half]),
            (matrix_in.at[matrix_half], matrices.at[section, matrix_half]),
        ]
        return [
            pltpu.make_async_remote_copy(
                src_ref=source, dst_ref=target_ref, send_sem=weight_sent.at[i, target],
                recv_sem=weight_got.at[i, section], device_id={"section": target},
                device_id_type=MESH,
            )
            for i, (source, target_ref) in enumerate(refs)
        ]

    def send_weights():
        for i in range(3):
            for target in range(IDLE, SECTIONS):

                @pl.when(section != target)
                def _():
                    weight_copies(target)[i].start()

    def arrived(i, block):
        refs = [
            gains.at[block],
            filters.at[block, filter_half],
            matrices.at[block, matrix_half],
        ]
        pltpu.make_async_copy(refs[i], refs[i], weight_got.at[i, block]).wait()

    def share(i, block):
        ref = filters.at[block, filter_half] if i == 0 else matrices.at[block, matrix_half]
        return pltpu.make_async_remote_copy(
            src_ref=ref, dst_ref=ref, send_sem=share_sent.at[i], recv_sem=share_got.at[i, block],
            device_id={"sht": sibling}, device_id_type=MESH,
        )

    @pl.when(section == 0)
    def _():
        send_weights()

    @pl.when(section == 1)
    def _():
        pl.semaphore_wait(pace, 1)
        send_weights()

    def exchange(send, recv, sent, got):
        recv[me] = send[me]

        def one(t, carry):
            to = lax.rem(me + t, SHT)
            pltpu.make_async_remote_copy(
                src_ref=send.at[to], dst_ref=recv.at[me], send_sem=sent, recv_sem=got,
                device_id={"sht": to}, device_id_type=MESH,
            ).start()
            return carry

        lax.fori_loop(1, SHT, one, 0)

    def wait_all(buffer, semaphore):
        ref = buffer.at[pl.ds(0, SHT - 1)]
        pltpu.make_async_copy(ref, ref, semaphore).wait()

    def out_copy(lat, slot, member, block):
        return pltpu.make_async_remote_copy(
            src_ref=leaving.at[slot, lat], dst_ref=out.at[member, lat],
            send_sem=out_sent.at[slot, lat], recv_sem=out_got.at[member, lat],
            device_id={"section": block}, device_id_type=MESH,
        )

    def own_copy(lat, slot, member):
        return pltpu.make_async_copy(
            leaving.at[slot, lat], out.at[member, lat], out_sent.at[slot, lat]
        )

    def wait_left(lat, slot):
        ref = leaving.at[slot, lat]
        pltpu.make_async_copy(ref, ref, out_sent.at[slot, lat]).wait()

    low = lane_of((HALF, HALF)) < HALF // 2
    low_all = lane_of((NLON, HALF)) < HALF // 2

    def step(block, carry):
        away = section != block

        @pl.when(section == block + 2)
        def _():
            send_weights()

        @pl.when(away)
        def _():
            arrived(0, block)

        for lat in range(2):
            wide = layer_norm(state[lat].astype(F32), gains[block, 0:1, :])
            narrow = wide.astype(BF)
            normed[lat] = narrow
            turned = pltpu.roll(wide[:, HALF:], HALF // 2, 1).astype(BF)
            real = dot(fourier[0], narrow)
            imag = dot(fourier[1], jnp.concatenate([narrow[:, :HALF], turned], axis=1))
            spectrum = jnp.concatenate(
                [real[:, :HALF], imag[:, :HALF], real[:, HALF:] + imag[:, HALF:]], axis=1
            ).astype(BF)
            send_one[:, 2 * lat : 2 * lat + 2, :] = spectrum.reshape(SHT, 2, 2 * C)
        exchange(send_one, recv_one, sent_one, got_one)

        @pl.when(away)
        def _():
            arrived(1, block)
            share(0, block).start()

        wait_all(recv_one, got_one)
        coeffs = dot(legendre[...], recv_one[...].reshape(2 * NLAT, 2 * C))

        @pl.when(away)
        def _():
            share(0, block).wait()

        gain = filters[block].astype(F32)
        gain_real, gain_imag = gain[:, :HALF], gain[:, HALF : 2 * HALF]
        gain_rest = gain[:, 2 * HALF :]
        gain_turned = pltpu.roll(gain_rest, HALF // 2, 1)
        gain_straight = jnp.where(low, gain_rest, gain_turned)
        gain_cross = jnp.where(low, -gain_turned, gain_rest)
        parts = []
        for order in range(2):
            part = coeffs[order * LMAX : (order + 1) * LMAX]
            real, imag, rest = part[:, :HALF], part[:, HALF : 2 * HALF], part[:, 2 * HALF :]
            parts.append(
                jnp.concatenate(
                    [
                        real * gain_real - imag * gain_imag,
                        real * gain_imag + imag * gain_real,
                        rest * gain_straight + pltpu.roll(rest, HALF // 2, 1) * gain_cross,
                    ],
                    axis=1,
                )
            )
        filtered = jnp.concatenate(parts, axis=0).astype(BF)
        returned = dot(legendre_back[...], filtered).astype(BF)

        wait_all(send_one, sent_one)

        send_two[...] = returned.reshape(SHT, 4, 2 * C)
        exchange(send_two, recv_two, sent_two, got_two)

        @pl.when(away)
        def _():
            arrived(2, block)
            copy = share(1, block)
            copy.start()
            copy.wait()

        @pl.when(jnp.logical_and(block == 0, section == 4))
        def _():
            pl.semaphore_signal(pace, inc=1, device_id={"section": 1}, device_id_type=MESH)

        skip = matrices[block, :, 0:PAD]
        into = matrices[block, :, PAD : PAD + HID]
        back = matrices[block, :, PAD + HID :]
        for lat in range(2):
            skipped[lat] = dot(normed[lat], skip)

        wait_all(recv_two, got_two)
        slot = lax.rem(block, 2)
        for lat in range(2):
            waves = recv_two[:, 2 * lat : 2 * lat + 2, :].reshape(MMAX, 2 * C)
            rest = waves[:, 2 * HALF :].astype(F32)
            top = jnp.where(low, rest, 0.0).astype(BF)
            bottom = jnp.where(low, pltpu.roll(rest, HALF // 2, 1), 0.0).astype(BF)
            stacked = jnp.concatenate(
                [
                    jnp.concatenate([waves[:, :HALF], top], axis=1),
                    jnp.concatenate([waves[:, HALF : 2 * HALF], bottom], axis=1),
                ],
                axis=0,
            )
            activated = gelu(dot(inverse_fourier[...], stacked) + skipped[lat])
            second = layer_norm(activated, gains[block, 1:2, :]).astype(BF)
            hidden = gelu(dot(second, into)).astype(BF)
            update = lax.dot_general(
                hidden, back, (((1,), (1,)), ((), ())), preferred_element_type=F32
            )
            result = state[lat].astype(F32) + update
            state[lat] = result.astype(BF)

            @pl.when(block >= 2)
            def _():
                wait_left(lat, slot)

            odd = pltpu.roll(result[NLON // 2 :, :HALF], HALF // 2, 1)
            odd_rest = pltpu.roll(result[NLON // 2 :, HALF:], HALF // 2, 1)
            leaving[slot, lat] = jnp.concatenate(
                [
                    result[: NLON // 2, :HALF],
                    jnp.where(low, result[: NLON // 2, HALF:], odd),
                    jnp.where(low, odd, odd_rest),
                ],
                axis=1,
            ).astype(BF)

            @pl.when(away)
            def _():
                out_copy(lat, slot, section - IDLE, block).start()

            @pl.when(jnp.logical_not(away))
            def _():
                own_copy(lat, slot, section - IDLE).start()

        wait_all(send_two, sent_two)
        return carry

    @pl.when(section >= IDLE)
    def _():
        lax.fori_loop(0, SECTIONS, step, 0)
        for slot in range(2):
            for lat in range(2):
                wait_left(lat, slot)

    for target in range(IDLE, SECTIONS):

        @pl.when(section != target)
        def _():
            for copy in weight_copies(target):
                copy.wait_send()

    for member in range(MEMBERS):

        @pl.when(section != member + IDLE)
        def _():
            for lat in range(2):
                ref = out.at[member, lat]
                pltpu.make_async_copy(ref, ref, out_got.at[member, lat]).wait()


def per_device(
    analysis, perturbations, gain_first, spectral_gain, skip_weight, gain_second, mlp_in, mlp_out
):
    wide = perturbations.astype(F32)
    average = jnp.mean(wide, axis=0, keepdims=True)
    members = (analysis.astype(F32)[None] + wide - average).astype(BF)
    members = jnp.pad(members, ((IDLE, 0), (0, 0), (0, 0), (0, 0)))
    slices = lax.all_to_all(members, "section", split_axis=0, concat_axis=0, tiled=True)
    lats = slices.shape[1]
    begin = slices.reshape(SECTIONS, lats, NLON // 2, 2, C // SECTIONS)
    begin = jnp.transpose(begin, (1, 3, 2, 0, 4)).reshape(lats, NLON, C)
    begin = jnp.pad(begin, ((0, 0), (0, 0), (0, PAD - C)))

    gains = jnp.pad(
        jnp.concatenate([gain_first, gain_second], axis=0), ((0, 6), (0, PAD - C))
    )
    g = spectral_gain[0].astype(BF).reshape(2, LMAX, C)
    filters = jnp.concatenate([g[0, :, :HALF], g[1, :, :HALF], g[0, :, HALF:], g[1, :, HALF:]], axis=1)
    matrices = jnp.concatenate(
        [jnp.pad(skip_weight[0], ((0, 0), (0, PAD - C))), mlp_in[0], mlp_out[0]], axis=1
    )
    forward, inverse = longitude_tables()
    vmem = pl.BlockSpec(memory_space=pltpu.VMEM)
    out = pl.pallas_call(
        kernel,
        out_shape=jax.ShapeDtypeStruct((MEMBERS, lats, NLON // 2, 2 * C), BF),
        in_specs=[vmem] * 7,
        out_specs=pl.BlockSpec(memory_space=pl.ANY),
        scratch_shapes=[
            pltpu.VMEM((2, NLON, PAD), BF),
            pltpu.VMEM((2, NLON, PAD), BF),
            pltpu.VMEM((2, NLON, PAD), F32),
            pltpu.VMEM((SHT, 4, 2 * C), BF),
            pltpu.VMEM((SHT, 4, 2 * C), BF),
            pltpu.VMEM((SHT, 4, 2 * C), BF),
            pltpu.VMEM((SHT, 4, 2 * C), BF),
            pltpu.VMEM((SECTIONS, 8, PAD), F32),
            pltpu.VMEM((SECTIONS, LMAX, 2 * C), BF),
            pltpu.VMEM((SECTIONS, PAD, 1024), BF),
            pltpu.VMEM((LMAX, 2 * NLAT), F32),
            pltpu.VMEM((LMAX, 2 * NLAT), F32),
            pltpu.VMEM((LMAX, 2 * NLAT), F32),
            pltpu.VMEM((LMAX, 2 * NLAT), F32),
            pltpu.VMEM((2 * LMAX, 2 * NLAT), BF),
            pltpu.VMEM((2 * NLAT, 2 * LMAX), BF),
            pltpu.VMEM((2, 2, NLON // 2, 2 * C), BF),
            pltpu.SemaphoreType.DMA,
            pltpu.SemaphoreType.DMA,
            pltpu.SemaphoreType.DMA,
            pltpu.SemaphoreType.DMA,
            pltpu.SemaphoreType.DMA((3, SECTIONS)),
            pltpu.SemaphoreType.DMA((3, SECTIONS)),
            pltpu.SemaphoreType.DMA((2,)),
            pltpu.SemaphoreType.DMA((2, SECTIONS)),
            pltpu.SemaphoreType.DMA((2, 2)),
            pltpu.SemaphoreType.DMA((MEMBERS, 2)),
            pltpu.SemaphoreType.REGULAR,
        ],
        compiler_params=pltpu.CompilerParams(
            collective_id=0, has_side_effects=True, vmem_limit_bytes=40 * 1024 * 1024
        ),
    )(begin, gains, filters, matrices, forward, inverse, latitude_rows())
    return out.reshape(1, MEMBERS, lats, NLON * C)


def solution(mesh):
    return jax.shard_map(
        per_device,
        mesh=mesh,
        in_specs=(
            P("sht", None, "section"),
            P(None, "sht", None, "section"),
            P("section", None),
            P("section", None, None),
            P("section", None, None),
            P("section", None),
            P("section", None, None),
            P("section", None, None),
        ),
        out_specs=P("section", None, "sht", None),
        check_vma=False,
    )
```

```python
import math

import jax
import jax.numpy as jnp
import numpy as np
from jax import lax
from jax.experimental import pallas as pl
from jax.experimental.pallas import tpu as pltpu
from jax.sharding import PartitionSpec as P

C = 192
HID = 384
NLAT = 128
NLON = 256
LMAX = 128
MMAX = 128
MEMBERS = 6
SECTIONS = 8
SHT = 64
IDLE = 2
PAD = 256
HALF = 128
MESH = pl.DeviceIdType.MESH
BF = jnp.bfloat16
F32 = jnp.float32


def partner_offsets():
    hops = lambda o: min(o[0], 4 - o[0]) + min(o[1], 8 - o[1])
    offsets = [(dx, dy) for dx in range(4) for dy in range(8)]
    return sorted(offsets, key=lambda o: (-hops(o), o[1] % 2, o[0]))


def longitude_tables():
    order = np.concatenate([np.arange(0, NLON, 2), np.arange(1, NLON, 2)])
    waves = np.arange(MMAX)
    phase = (waves[:, None] * order[None, :] % NLON).astype(np.float32) * np.float32(
        2.0 * math.pi / NLON
    )
    cosines = np.cos(phase)
    sines = np.sin(phase)
    forward = np.stack([cosines, -sines])
    factor = np.where(waves == 0, 1.0, 2.0).astype(np.float32)
    inverse = np.concatenate([cosines.T * factor, -sines.T * factor], axis=1)
    return jnp.asarray(forward, BF), jnp.asarray(inverse, BF)


def latitude_rows():
    lane = np.arange(2 * NLAT)
    colatitude = (math.pi * (lane // 2 + 0.5) / NLAT).astype(np.float32)
    sine = np.sin(colatitude)
    rows = np.zeros((8, 2 * NLAT), np.float32)
    rows[0] = np.cos(colatitude)
    rows[1] = sine
    rows[2] = np.log(sine)
    rows[3] = sine * (2.0 * math.pi / NLON) * (math.pi / NLAT)
    rows[4] = lane % 2
    return jnp.asarray(rows)


def gelu(x):
    return 0.5 * x * (1.0 + lax.erf(x * math.sqrt(0.5)))


def lane_of(shape):
    return lax.broadcasted_iota(jnp.int32, shape, len(shape) - 1)


def layer_norm(values, gain_row):
    average = jnp.sum(values, axis=1, keepdims=True) * (1.0 / C)
    centred = jnp.where(lane_of(values.shape) < C, values - average, 0.0)
    variance = jnp.sum(centred * centred, axis=1, keepdims=True) * (1.0 / C)
    return centred * lax.rsqrt(variance + 1e-05) * gain_row


def dot(a, b):
    return jnp.dot(a, b, preferred_element_type=F32)


def build_legendre(me, rows_ref, lower, upper, first, table, forward_table, inverse_table):
    cosine = rows_ref[0:1, :]
    parity = rows_ref[4:5, :]
    order = parity + (2 * me).astype(F32)
    shape = (LMAX, 2 * NLAT)
    degree = lax.broadcasted_iota(jnp.int32, shape, 0).astype(F32)
    step = degree + 1.0
    terms = jnp.where(step <= order, 0.5 * jnp.log((2.0 * step + 1.0) / (2.0 * step)), 0.0)
    picked = jnp.sum(terms, axis=0, keepdims=True)
    diagonal = jnp.exp(picked + order * rows_ref[2:3, :]) * math.sqrt(0.25 / math.pi)
    lower[...] = jnp.sqrt(
        jnp.maximum(4.0 * degree * degree - 1.0, 0.0)
        / jnp.maximum(degree * degree - order * order, 1.0)
    )
    shifted = degree - 1.0
    upper[...] = jnp.sqrt(
        jnp.maximum(shifted * shifted - order * order, 0.0)
        / jnp.maximum(4.0 * shifted * shifted - 1.0, 1.0)
    )
    first[...] = jnp.where(degree == order, diagonal, 0.0)

    def advance(row, carry):
        latest, earlier = carry
        at = pl.ds(row, 1)
        current = lower[at, :] * (cosine * latest - upper[at, :] * earlier) + first[at, :]
        table[pl.ds(lax.rem(row, 2) * (LMAX // 2) + row // 2, 1), :] = current
        return (current, latest)

    zero = cosine * 0.0
    lax.fori_loop(0, LMAX, advance, (zero, zero), unroll=8)
    plain = table[...]
    weighted = plain * rows_ref[3:4, :]
    even = jnp.broadcast_to(parity, shape) < 0.5
    forward_table[0:LMAX, :] = jnp.where(even, weighted, 0.0).astype(BF)
    forward_table[LMAX:, :] = jnp.where(even, 0.0, weighted).astype(BF)
    inverse_table[:, 0:LMAX] = jnp.where(even, plain, 0.0).T.astype(BF)
    inverse_table[:, LMAX:] = jnp.where(even, 0.0, plain).T.astype(BF)


def kernel(
    analysis, perturbations, gain_first, gain_second, gain_tiles, skip_in, mlp_in, mlp_out,
    fourier, inverse_fourier, rows,
    out,
    outgoing, begin, stage, state, normed, skipped, send_one, send_two, recv_one, recv_two,
    gains, filters, matrices, lower, upper, first, table, legendre, legendre_back, leaving,
    sent_one, sent_two, got_one, got_two, weight_sent, weight_got,
    share_sent, share_got, out_sent, out_got, member_sent, member_got, pace,
):
    section = lax.axis_index("section")
    me = lax.axis_index("sht")
    core = lax.rem(me, 2)
    sibling = me + 1 - 2 * core
    chip_x = me // 16
    chip_y = lax.rem(me // 2, 8)

    barrier = pltpu.get_barrier_semaphore()

    def greet(t, carry):
        pl.semaphore_signal(
            barrier, inc=1, device_id={"sht": lax.rem(me + t, SHT)}, device_id_type=MESH
        )
        return carry

    def greet_column(t, carry):
        pl.semaphore_signal(
            barrier, inc=1, device_id={"section": lax.rem(section + t, SECTIONS)},
            device_id_type=MESH,
        )
        return carry

    lax.fori_loop(1, SHT, greet, 0)
    lax.fori_loop(1, SECTIONS, greet_column, 0)

    deviations = perturbations[...].astype(F32)
    average = jnp.sum(deviations, axis=0) * (1.0 / MEMBERS)
    centre = analysis[...].astype(F32)
    for member in range(MEMBERS):
        outgoing[member] = (centre + deviations[member] - average).astype(BF)

    gains[section] = jnp.zeros((8, PAD), F32)
    gains[section, 0:1, 0:C] = gain_first[...]
    gains[section, 1:2, 0:C] = gain_second[...]
    tiles = [[gain_tiles[:, third, p, :] for third in range(3)] for p in range(2)]
    turned = [[pltpu.roll(tile, HALF // 2, 1) for tile in row] for row in tiles]
    left = lane_of((LMAX // 2, HALF)) < HALF // 2
    even_rows, odd_rows = pl.ds(0, LMAX // 2), pl.ds(LMAX // 2, LMAX // 2)
    for p in range(2):
        at = pl.ds(p * HALF, HALF)
        filters[section, even_rows, at] = tiles[p][0].astype(BF)
        filters[section, odd_rows, at] = jnp.where(left, turned[p][1], turned[p][2]).astype(BF)
    at = pl.ds(2 * HALF, HALF)
    filters[section, even_rows, at] = jnp.where(left, tiles[0][1], turned[1][1]).astype(BF)
    filters[section, odd_rows, at] = jnp.where(left, turned[0][2], tiles[1][2]).astype(BF)
    matrices[:, C:, :] = jnp.zeros((SECTIONS, PAD - C, 1024), BF)
    matrices[section, 0:C, 0:PAD] = jnp.concatenate(
        [skip_in[...], jnp.zeros((C, PAD - C), BF)], axis=1
    )
    matrices[section, 0:C, PAD : PAD + HID] = mlp_in[...]
    matrices[section, 0:C, PAD + HID :] = mlp_out[...]

    pl.semaphore_wait(barrier, SHT - 1 + SECTIONS - 1)

    def member_copy(member):
        return pltpu.make_async_remote_copy(
            src_ref=outgoing.at[member], dst_ref=begin.at[section],
            send_sem=member_sent.at[member], recv_sem=member_got,
            device_id={"section": member + IDLE}, device_id_type=MESH,
        )

    for member in range(MEMBERS):

        @pl.when(section != member + IDLE)
        def _():
            member_copy(member).start()

    filter_half = pl.ds(pl.multiple_of(core * (LMAX // 2), LMAX // 2), LMAX // 2)
    matrix_half = pl.ds(pl.multiple_of(core * (C // 2), C // 2), C // 2)

    def weight_copy(i, target):
        ref = [
            gains.at[section],
            filters.at[section, filter_half],
            matrices.at[section, matrix_half],
        ][i]
        return pltpu.make_async_remote_copy(
            src_ref=ref, dst_ref=ref, send_sem=weight_sent.at[i, target],
            recv_sem=weight_got.at[i, section], device_id={"section": target},
            device_id_type=MESH,
        )

    def send_weights(i):
        for target in range(IDLE, SECTIONS):

            @pl.when(section != target)
            def _():
                weight_copy(i, target).start()

    def arrived(i, block):
        ref = [
            gains.at[block],
            filters.at[block, filter_half],
            matrices.at[block, matrix_half],
        ][i]
        pltpu.make_async_copy(ref, ref, weight_got.at[i, block]).wait()

    def share(i, block):
        ref = filters.at[block, filter_half] if i == 0 else matrices.at[block, matrix_half]
        return pltpu.make_async_remote_copy(
            src_ref=ref, dst_ref=ref, send_sem=share_sent.at[i], recv_sem=share_got.at[i, block],
            device_id={"sht": sibling}, device_id_type=MESH,
        )

    send_weights(0)

    @pl.when(section < IDLE)
    def _():
        send_weights(1)

    @pl.when(section == 1)
    def _():
        pl.semaphore_wait(pace, 1)

    @pl.when(section < IDLE)
    def _():
        send_weights(2)

    def exchange(send, recv, sent, got):
        recv[me] = send[me]
        for dx, dy in partner_offsets():
            base = lax.rem(chip_x + dx, 4) * 16 + lax.rem(chip_y + dy, 8) * 2
            for turn in (0, 1) if dx or dy else (1,):
                to = base + lax.rem(core + turn, 2)
                pltpu.make_async_remote_copy(
                    src_ref=send.at[to], dst_ref=recv.at[me], send_sem=sent, recv_sem=got,
                    device_id={"sht": to}, device_id_type=MESH,
                ).start()

    def wait_all(buffer, semaphore):
        ref = buffer.at[pl.ds(0, SHT - 1)]
        pltpu.make_async_copy(ref, ref, semaphore).wait()

    def out_copy(lat, slot, member, block):
        return pltpu.make_async_remote_copy(
            src_ref=leaving.at[slot, lat], dst_ref=out.at[member, lat],
            send_sem=out_sent.at[slot, lat], recv_sem=out_got.at[member, lat],
            device_id={"section": block}, device_id_type=MESH,
        )

    def own_copy(lat, slot, member):
        return pltpu.make_async_copy(
            leaving.at[slot, lat], out.at[member, lat], out_sent.at[slot, lat]
        )

    def wait_left(lat, slot):
        ref = leaving.at[slot, lat]
        pltpu.make_async_copy(ref, ref, out_sent.at[slot, lat]).wait()

    low = lane_of((HALF, HALF)) < HALF // 2
    low_all = lane_of((NLON, HALF)) < HALF // 2

    def step(block, carry):
        away = section != block

        @pl.when(section == block + 2)
        def _():
            send_weights(1)
            send_weights(2)

        @pl.when(away)
        def _():
            arrived(0, block)

        for lat in range(2):
            wide = layer_norm(state[lat].astype(F32), gains[block, 0:1, :])
            narrow = wide.astype(BF)
            normed[lat] = narrow
            turned = pltpu.roll(wide[:, HALF:], HALF // 2, 1).astype(BF)
            real = dot(fourier[0], narrow)
            imag = dot(fourier[1], jnp.concatenate([narrow[:, :HALF], turned], axis=1))
            spectrum = jnp.concatenate(
                [real[:, :HALF], imag[:, :HALF], real[:, HALF:] + imag[:, HALF:]], axis=1
            ).astype(BF)
            send_one[:, 2 * lat : 2 * lat + 2, :] = spectrum.reshape(SHT, 2, 2 * C)
        exchange(send_one, recv_one, sent_one, got_one)

        @pl.when(away)
        def _():
            arrived(1, block)
            share(0, block).start()

        wait_all(recv_one, got_one)
        coeffs = dot(legendre[...], recv_one[...].reshape(2 * NLAT, 2 * C))

        @pl.when(away)
        def _():
            share(0, block).wait()

        gain = filters[block].astype(F32)
        gain_real, gain_imag = gain[:, :HALF], gain[:, HALF : 2 * HALF]
        gain_rest = gain[:, 2 * HALF :]
        gain_turned = pltpu.roll(gain_rest, HALF // 2, 1)
        gain_straight = jnp.where(low, gain_rest, gain_turned)
        gain_cross = jnp.where(low, -gain_turned, gain_rest)
        parts = []
        for order in range(2):
            part = coeffs[order * LMAX : (order + 1) * LMAX]
            real, imag, rest = part[:, :HALF], part[:, HALF : 2 * HALF], part[:, 2 * HALF :]
            parts.append(
                jnp.concatenate(
                    [
                        real * gain_real - imag * gain_imag,
                        real * gain_imag + imag * gain_real,
                        rest * gain_straight + pltpu.roll(rest, HALF // 2, 1) * gain_cross,
                    ],
                    axis=1,
                )
            )
        filtered = jnp.concatenate(parts, axis=0).astype(BF)
        returned = dot(legendre_back[...], filtered).astype(BF)

        wait_all(send_one, sent_one)

        send_two[...] = returned.reshape(SHT, 4, 2 * C)
        exchange(send_two, recv_two, sent_two, got_two)

        @pl.when(away)
        def _():
            arrived(2, block)
            copy = share(1, block)
            copy.start()
            copy.wait()

        @pl.when(jnp.logical_and(block == 0, section == 4))
        def _():
            pl.semaphore_signal(pace, inc=1, device_id={"section": 1}, device_id_type=MESH)

        skip = matrices[block, :, 0:PAD]
        into = matrices[block, :, PAD : PAD + HID]
        back = matrices[block, :, PAD + HID :]
        for lat in range(2):
            skipped[lat] = dot(normed[lat], skip)

        wait_all(recv_two, got_two)
        slot = lax.rem(block, 2)
        for lat in range(2):
            waves = recv_two[:, 2 * lat : 2 * lat + 2, :].reshape(MMAX, 2 * C)
            rest = waves[:, 2 * HALF :].astype(F32)
            top = jnp.where(low, rest, 0.0).astype(BF)
            bottom = jnp.where(low, pltpu.roll(rest, HALF // 2, 1), 0.0).astype(BF)
            stacked = jnp.concatenate(
                [
                    jnp.concatenate([waves[:, :HALF], top], axis=1),
                    jnp.concatenate([waves[:, HALF : 2 * HALF], bottom], axis=1),
                ],
                axis=0,
            )
            activated = gelu(dot(inverse_fourier[...], stacked) + skipped[lat])
            second = layer_norm(activated, gains[block, 1:2, :]).astype(BF)
            hidden = gelu(dot(second, into)).astype(BF)
            update = lax.dot_general(
                hidden, back, (((1,), (1,)), ((), ())), preferred_element_type=F32
            )
            result = state[lat].astype(F32) + update
            state[lat] = result.astype(BF)

            @pl.when(block >= 2)
            def _():
                wait_left(lat, slot)

            odd = pltpu.roll(result[NLON // 2 :, :HALF], HALF // 2, 1)
            odd_rest = pltpu.roll(result[NLON // 2 :, HALF:], HALF // 2, 1)
            leaving[slot, lat] = jnp.concatenate(
                [
                    result[: NLON // 2, :HALF],
                    jnp.where(low, result[: NLON // 2, HALF:], odd),
                    jnp.where(low, odd, odd_rest),
                ],
                axis=1,
            ).astype(BF)

            @pl.when(away)
            def _():
                out_copy(lat, slot, section - IDLE, block).start()

            @pl.when(jnp.logical_not(away))
            def _():
                own_copy(lat, slot, section - IDLE).start()

        wait_all(send_two, sent_two)
        return carry

    @pl.when(section >= IDLE)
    def _():
        begin[section] = outgoing[section - IDLE]
        build_legendre(me, rows, lower, upper, first, table, legendre, legendre_back)
        slots = begin.at[pl.ds(0, SECTIONS - 1)]
        pltpu.make_async_copy(slots, slots, member_got).wait()
        for lat in range(2):
            grid = begin[:, lat].astype(F32).reshape(C, NLON).T
            for tile in range(2):
                part = grid[:, :HALF]
                if tile:
                    part = jnp.concatenate(
                        [grid[:, HALF:], jnp.zeros((NLON, PAD - C), F32)], axis=1
                    )
                stage[tile] = part
                for odd in range(2):
                    rows_of = pl.ds(odd * HALF, HALF)
                    state[lat, rows_of, pl.ds(tile * HALF, HALF)] = stage[
                        tile, pl.ds(odd, HALF, stride=2), :
                    ].astype(BF)
        lax.fori_loop(0, SECTIONS, step, 0)
        for slot in range(2):
            for lat in range(2):
                wait_left(lat, slot)

    for target in range(IDLE, SECTIONS):

        @pl.when(section != target)
        def _():
            for i in range(3):
                weight_copy(i, target).wait_send()

    for member in range(MEMBERS):

        @pl.when(section != member + IDLE)
        def _():
            member_copy(member).wait_send()
            for lat in range(2):
                ref = out.at[member, lat]
                pltpu.make_async_copy(ref, ref, out_got.at[member, lat]).wait()


def per_device(
    analysis, perturbations, gain_first, spectral_gain, skip_weight, gain_second, mlp_in, mlp_out
):
    lats = analysis.shape[0]
    tiles = spectral_gain[0].reshape(2, LMAX // 2, 3, HALF)
    forward, inverse = longitude_tables()
    vmem = pl.BlockSpec(memory_space=pltpu.VMEM)
    out = pl.pallas_call(
        kernel,
        out_shape=jax.ShapeDtypeStruct((MEMBERS, lats, NLON // 2, 2 * C), BF),
        in_specs=[vmem] * 11,
        out_specs=pl.BlockSpec(memory_space=pl.ANY),
        scratch_shapes=[
            pltpu.VMEM((MEMBERS, lats, C // SECTIONS, NLON), BF),
            pltpu.VMEM((SECTIONS, lats, C // SECTIONS, NLON), BF),
            pltpu.VMEM((2, NLON, HALF), F32),
            pltpu.VMEM((2, NLON, PAD), BF),
            pltpu.VMEM((2, NLON, PAD), BF),
            pltpu.VMEM((2, NLON, PAD), F32),
            pltpu.VMEM((SHT, 4, 2 * C), BF),
            pltpu.VMEM((SHT, 4, 2 * C), BF),
            pltpu.VMEM((SHT, 4, 2 * C), BF),
            pltpu.VMEM((SHT, 4, 2 * C), BF),
            pltpu.VMEM((SECTIONS, 8, PAD), F32),
            pltpu.VMEM((SECTIONS, LMAX, 2 * C), BF),
            pltpu.VMEM((SECTIONS, PAD, 1024), BF),
            pltpu.VMEM((LMAX, 2 * NLAT), F32),
            pltpu.VMEM((LMAX, 2 * NLAT), F32),
            pltpu.VMEM((LMAX, 2 * NLAT), F32),
            pltpu.VMEM((LMAX, 2 * NLAT), F32),
            pltpu.VMEM((2 * LMAX, 2 * NLAT), BF),
            pltpu.VMEM((2 * NLAT, 2 * LMAX), BF),
            pltpu.VMEM((2, 2, NLON // 2, 2 * C), BF),
            pltpu.SemaphoreType.DMA,
            pltpu.SemaphoreType.DMA,
            pltpu.SemaphoreType.DMA,
            pltpu.SemaphoreType.DMA,
            pltpu.SemaphoreType.DMA((3, SECTIONS)),
            pltpu.SemaphoreType.DMA((3, SECTIONS)),
            pltpu.SemaphoreType.DMA((2,)),
            pltpu.SemaphoreType.DMA((2, SECTIONS)),
            pltpu.SemaphoreType.DMA((2, 2)),
            pltpu.SemaphoreType.DMA((MEMBERS, 2)),
            pltpu.SemaphoreType.DMA((MEMBERS,)),
            pltpu.SemaphoreType.DMA,
            pltpu.SemaphoreType.REGULAR,
        ],
        compiler_params=pltpu.CompilerParams(
            collective_id=0, has_side_effects=True, vmem_limit_bytes=40 * 1024 * 1024
        ),
    )(
        jnp.transpose(analysis, (0, 2, 1)),
        jnp.transpose(perturbations, (0, 1, 3, 2)),
        gain_first,
        gain_second,
        jnp.transpose(tiles, (1, 2, 0, 3)),
        skip_weight[0],
        mlp_in[0],
        mlp_out[0],
        forward,
        inverse,
        latitude_rows(),
    )
    return out.reshape(1, MEMBERS, lats, NLON * C)


def solution(mesh):
    return jax.shard_map(
        per_device,
        mesh=mesh,
        in_specs=(
            P("sht", None, "section"),
            P(None, "sht", None, "section"),
            P("section", None),
            P("section", None, None),
            P("section", None, None),
            P("section", None),
            P("section", None, None),
            P("section", None, None),
        ),
        out_specs=P("section", None, "sht", None),
        check_vma=False,
    )
```

```python
import math

import jax
import jax.numpy as jnp
import numpy as np
from jax import lax
from jax.experimental import pallas as pl
from jax.experimental.pallas import tpu as pltpu
from jax.sharding import PartitionSpec as P

C = 192
HID = 384
NLAT = 128
NLON = 256
LMAX = 128
MMAX = 128
MEMBERS = 6
SECTIONS = 8
SHT = 64
HOME = (5, 6, 7, 0, 1, 2)
PAD = 256
HALF = 128
MESH = pl.DeviceIdType.MESH
BF = jnp.bfloat16
F32 = jnp.float32


def partner_offsets():
    hops = lambda o: min(o[0], 4 - o[0]) + min(o[1], 8 - o[1])
    offsets = [(dx, dy) for dx in range(4) for dy in range(8)]
    return sorted(offsets, key=lambda o: (-hops(o), o[1] % 2, o[0]))


def partners(chip_x, chip_y, core):
    for dx, dy in partner_offsets():
        base = lax.rem(chip_x + dx, 4) * 16 + lax.rem(chip_y + dy, 8) * 2
        for turn in (0, 1) if dx or dy else (1,):
            yield base + lax.rem(core + turn, 2)


def longitude_tables():
    order = np.concatenate([np.arange(0, NLON, 2), np.arange(1, NLON, 2)])
    waves = np.arange(MMAX)
    phase = (waves[:, None] * order[None, :] % NLON).astype(np.float32) * np.float32(
        2.0 * math.pi / NLON
    )
    cosines = np.cos(phase)
    sines = np.sin(phase)
    forward = np.stack([cosines, -sines])
    factor = np.where(waves == 0, 1.0, 2.0).astype(np.float32)
    inverse = np.concatenate([cosines.T * factor, -sines.T * factor], axis=1)
    return jnp.asarray(forward, BF), jnp.asarray(inverse, BF)


def latitude_rows():
    lane = np.arange(2 * NLAT)
    colatitude = (math.pi * (lane // 2 + 0.5) / NLAT).astype(np.float32)
    sine = np.sin(colatitude)
    rows = np.zeros((8, 2 * NLAT), np.float32)
    rows[0] = np.cos(colatitude)
    rows[1] = sine
    rows[2] = np.log(sine)
    rows[3] = sine * (2.0 * math.pi / NLON) * (math.pi / NLAT)
    rows[4] = lane % 2
    return jnp.asarray(rows)


def gelu(x):
    return 0.5 * x * (1.0 + lax.erf(x * math.sqrt(0.5)))


def lane_of(shape):
    return lax.broadcasted_iota(jnp.int32, shape, len(shape) - 1)


def layer_norm(values, gain_row):
    average = jnp.sum(values, axis=1, keepdims=True) * (1.0 / C)
    centred = jnp.where(lane_of(values.shape) < C, values - average, 0.0)
    variance = jnp.sum(centred * centred, axis=1, keepdims=True) * (1.0 / C)
    return centred * lax.rsqrt(variance + 1e-05) * gain_row


def dot(a, b):
    return jnp.dot(a, b, preferred_element_type=F32)


def build_legendre(me, rows_ref, lower, upper, first, table, forward_table, inverse_table):
    cosine = rows_ref[0:1, :]
    parity = rows_ref[4:5, :]
    order = parity + (2 * me).astype(F32)
    shape = (LMAX, 2 * NLAT)
    degree = lax.broadcasted_iota(jnp.int32, shape, 0).astype(F32)
    step = degree + 1.0
    terms = jnp.where(step <= order, 0.5 * jnp.log((2.0 * step + 1.0) / (2.0 * step)), 0.0)
    picked = jnp.sum(terms, axis=0, keepdims=True)
    diagonal = jnp.exp(picked + order * rows_ref[2:3, :]) * math.sqrt(0.25 / math.pi)
    lower[...] = jnp.sqrt(
        jnp.maximum(4.0 * degree * degree - 1.0, 0.0)
        / jnp.maximum(degree * degree - order * order, 1.0)
    )
    shifted = degree - 1.0
    upper[...] = jnp.sqrt(
        jnp.maximum(shifted * shifted - order * order, 0.0)
        / jnp.maximum(4.0 * shifted * shifted - 1.0, 1.0)
    )
    first[...] = jnp.where(degree == order, diagonal, 0.0)

    def advance(row, carry):
        latest, earlier = carry
        at = pl.ds(row, 1)
        current = lower[at, :] * (cosine * latest - upper[at, :] * earlier) + first[at, :]
        table[pl.ds(lax.rem(row, 2) * (LMAX // 2) + row // 2, 1), :] = current
        return (current, latest)

    zero = cosine * 0.0
    lax.fori_loop(0, LMAX, advance, (zero, zero), unroll=8)
    plain = table[...]
    weighted = plain * rows_ref[3:4, :]
    even = jnp.broadcast_to(parity, shape) < 0.5
    forward_table[0:LMAX, :] = jnp.where(even, weighted, 0.0).astype(BF)
    forward_table[LMAX:, :] = jnp.where(even, 0.0, weighted).astype(BF)
    inverse_table[:, 0:LMAX] = jnp.where(even, plain, 0.0).T.astype(BF)
    inverse_table[:, LMAX:] = jnp.where(even, 0.0, plain).T.astype(BF)


def kernel(
    analysis_in, perturbations_in, gain_first_in, gain_second_in, gain_tiles_in, skip_in,
    mlp_in, mlp_out, fourier_in, inverse_fourier_in, rows_in,
    out,
    analysis, perturbations, gain_first, gain_second, gain_tiles, skip_own,
    fourier, inverse_fourier, rows, loaded,
    outgoing, begin, stage, state, normed, skipped,
    send_one_main, send_two_main, recv_one_main, recv_two_main,
    send_one_rest, send_two_rest, recv_one_rest, recv_two_rest,
    gains, filters, matrices, lower, upper, first, table, legendre, legendre_back, leaving,
    sent, got, weight_sent, weight_got, pass_sent, pass_got,
    share_sent, share_got, out_sent, out_got, member_sent, member_got, pace,
):
    section = lax.axis_index("section")
    me = lax.axis_index("sht")
    core = lax.rem(me, 2)
    sibling = me + 1 - 2 * core
    own = lax.rem(section + 3, SECTIONS)
    holds = own < MEMBERS
    chip_x = me // 16
    chip_y = lax.rem(me // 2, 8)

    loads = [
        pltpu.make_async_copy(source, target, loaded.at[i])
        for i, (source, target) in enumerate(
            [
                (perturbations_in, perturbations),
                (analysis_in, analysis),
                (gain_first_in, gain_first),
                (gain_second_in, gain_second),
                (gain_tiles_in, gain_tiles),
                (skip_in, skip_own),
                (mlp_in, matrices.at[section, pl.ds(0, C), pl.ds(PAD, HID)]),
                (mlp_out, matrices.at[section, pl.ds(0, C), pl.ds(PAD + HID, HID)]),
                (rows_in, rows),
                (fourier_in, fourier),
                (inverse_fourier_in, inverse_fourier),
            ]
        )
    ]
    for load in loads:
        load.start()
    barrier = pltpu.get_barrier_semaphore()

    def greet_column(t, carry):
        pl.semaphore_signal(
            barrier, inc=1, device_id={"section": lax.rem(section + t, SECTIONS)},
            device_id_type=MESH,
        )
        return carry

    for to in partners(chip_x, chip_y, core):
        pl.semaphore_signal(barrier, inc=1, device_id={"sht": to}, device_id_type=MESH)
    lax.fori_loop(1, SECTIONS, greet_column, 0)

    loads[0].wait()
    loads[1].wait()
    deviations = perturbations[...].astype(F32)
    average = jnp.sum(deviations, axis=0) * (1.0 / MEMBERS)
    centre = analysis[...].astype(F32)
    for member in range(MEMBERS):
        outgoing[member] = (centre + deviations[member] - average).astype(BF)

    for load in loads[2:8]:
        load.wait()
    gains[section] = jnp.zeros((8, PAD), F32)
    gains[section, 0:1, 0:C] = gain_first[...]
    gains[section, 1:2, 0:C] = gain_second[...]
    tiles = [[gain_tiles[:, third, p, :] for third in range(3)] for p in range(2)]
    turned = [[pltpu.roll(tile, HALF // 2, 1) for tile in row] for row in tiles]
    left = lane_of((LMAX // 2, HALF)) < HALF // 2
    even_rows, odd_rows = pl.ds(0, LMAX // 2), pl.ds(LMAX // 2, LMAX // 2)
    for p in range(2):
        at = pl.ds(p * HALF, HALF)
        filters[section, even_rows, at] = tiles[p][0].astype(BF)
        filters[section, odd_rows, at] = jnp.where(left, turned[p][1], turned[p][2]).astype(BF)
    at = pl.ds(2 * HALF, HALF)
    filters[section, even_rows, at] = jnp.where(left, tiles[0][1], turned[1][1]).astype(BF)
    filters[section, odd_rows, at] = jnp.where(left, turned[0][2], tiles[1][2]).astype(BF)
    matrices[:, C:, :] = jnp.zeros((SECTIONS, PAD - C, 1024), BF)
    matrices[section, 0:C, 0:PAD] = jnp.concatenate(
        [skip_own[...], jnp.zeros((C, PAD - C), BF)], axis=1
    )
    for load in loads[8:]:
        load.wait()

    pl.semaphore_wait(barrier, SHT - 1 + SECTIONS - 1)

    def member_copy(member):
        return pltpu.make_async_remote_copy(
            src_ref=outgoing.at[member], dst_ref=begin.at[section],
            send_sem=member_sent.at[member], recv_sem=member_got,
            device_id={"section": HOME[member]}, device_id_type=MESH,
        )

    for member in range(MEMBERS):

        @pl.when(section != HOME[member])
        def _():
            member_copy(member).start()

    filter_half = pl.ds(pl.multiple_of(core * (LMAX // 2), LMAX // 2), LMAX // 2)
    matrix_half = pl.ds(pl.multiple_of(core * 512, 512), 512)
    filter_piece = pl.ds(pl.multiple_of(core * 64 + chip_x * 16, 16), 16)
    matrix_piece = pl.ds(pl.multiple_of(core * 512 + chip_x * HALF, HALF), HALF)

    def part_of(i, block, piece):
        if i == 0:
            return gains.at[block]
        if i == 1:
            return filters.at[block, filter_piece if piece else filter_half]
        return matrices.at[block, pl.ds(0, C), matrix_piece if piece else matrix_half]

    def weight_copy(i, target):
        ref = part_of(i, section, True)
        return pltpu.make_async_remote_copy(
            src_ref=ref, dst_ref=ref, send_sem=weight_sent.at[i, target],
            recv_sem=weight_got.at[i, section], device_id={"section": target},
            device_id_type=MESH,
        )

    def send_weights(i):
        for target in HOME:

            @pl.when(section != target)
            def _():
                weight_copy(i, target).start()

    def arrived(i, block):
        ref = part_of(i, block, True)
        pltpu.make_async_copy(ref, ref, weight_got.at[i, block]).wait()

    def share(i, block):
        ref = part_of(i, block, False)
        return pltpu.make_async_remote_copy(
            src_ref=ref, dst_ref=ref, send_sem=share_sent.at[i], recv_sem=share_got.at[i, block],
            device_id={"sht": sibling}, device_id_type=MESH,
        )

    def pass_along(i, block, step):
        ref = part_of(i, block, True)
        to = lax.rem(chip_x + step, 4) * 16 + lax.rem(me, 16)
        return pltpu.make_async_remote_copy(
            src_ref=ref, dst_ref=ref, send_sem=pass_sent.at[i, step],
            recv_sem=pass_got.at[i, block], device_id={"sht": to}, device_id_type=MESH,
        )

    def hand_out(block):
        for i in (1, 2):
            arrived(i, block)
            for step in range(1, 4):
                pass_along(i, block, step).start()

    def collect(i, block):
        ref = filters.at[0, pl.ds(0, 48)] if i == 1 else matrices.at[0, pl.ds(0, C), pl.ds(0, 384)]
        pltpu.make_async_copy(ref, ref, pass_got.at[i, block]).wait()
        for step in range(1, 4):
            pass_along(i, block, step).wait_send()

    send_weights(0)

    @pl.when(section == 0)
    def _():
        send_weights(1)
        send_weights(2)

    @pl.when(jnp.logical_not(holds))
    def _():
        pl.semaphore_wait(pace, 1)
        send_weights(1)
        send_weights(2)

    def exchange(send, recv, sent, got):
        recv[me] = send[me]
        for to in partners(chip_x, chip_y, core):
            pltpu.make_async_remote_copy(
                src_ref=send.at[to], dst_ref=recv.at[me], send_sem=sent, recv_sem=got,
                device_id={"sht": to}, device_id_type=MESH,
            ).start()

    def wait_all(buffer, semaphore):
        ref = buffer.at[pl.ds(0, SHT - 1)]
        pltpu.make_async_copy(ref, ref, semaphore).wait()

    def out_copy(lat, slot, member, block):
        return pltpu.make_async_remote_copy(
            src_ref=leaving.at[slot, lat], dst_ref=out.at[member, lat],
            send_sem=out_sent.at[slot, lat], recv_sem=out_got.at[member, lat],
            device_id={"section": block}, device_id_type=MESH,
        )

    def own_copy(lat, slot, member):
        return pltpu.make_async_copy(
            leaving.at[slot, lat], out.at[member, lat], out_sent.at[slot, lat]
        )

    def wait_left(lat, slot):
        ref = leaving.at[slot, lat]
        pltpu.make_async_copy(ref, ref, out_sent.at[slot, lat]).wait()

    low = lane_of((HALF, HALF)) < HALF // 2
    low_all = lane_of((NLON, HALF)) < HALF // 2

    def step(block, carry):
        away = section != block

        @pl.when(away)
        def _():
            arrived(0, block)

        for lat in range(2):
            wide = layer_norm(state[lat].astype(F32), gains[block, 0:1, :])
            narrow = wide.astype(BF)
            normed[lat] = narrow
            turned = pltpu.roll(wide[:, HALF:], HALF // 2, 1).astype(BF)
            real = dot(fourier[0], narrow)
            imag = dot(fourier[1], jnp.concatenate([narrow[:, :HALF], turned], axis=1))
            at = pl.ds(2 * lat, 2)
            main = jnp.concatenate([real[:, :HALF], imag[:, :HALF]], axis=1).astype(BF)
            rest = (real[:, HALF:] + imag[:, HALF:]).astype(BF)
            send_one_main[:, at, :] = main.reshape(SHT, 2, 2 * HALF)
            send_one_rest[:, at, :] = rest.reshape(SHT, 2, HALF)
        exchange(send_one_main, recv_one_main, sent.at[0], got.at[0])
        exchange(send_one_rest, recv_one_rest, sent.at[1], got.at[1])

        @pl.when(jnp.logical_and(away, block == 0))
        def _():
            hand_out(0)

        @pl.when(away)
        def _():
            collect(1, block)
            copy = share(1, block)
            copy.start()
            copy.wait()

        gain = filters[block].astype(F32)
        gain_real, gain_imag = gain[:, :HALF], gain[:, HALF : 2 * HALF]
        gain_rest = gain[:, 2 * HALF :]
        gain_turned = pltpu.roll(gain_rest, HALF // 2, 1)
        gain_straight = jnp.where(low, gain_rest, gain_turned)
        gain_cross = jnp.where(low, -gain_turned, gain_rest)

        wait_all(recv_one_main, got.at[0])
        coeffs = dot(legendre[...], recv_one_main[...].reshape(2 * NLAT, 2 * HALF))
        parts = []
        for order in range(2):
            part = coeffs[order * LMAX : (order + 1) * LMAX]
            real, imag = part[:, :HALF], part[:, HALF:]
            parts.append(
                jnp.concatenate(
                    [real * gain_real - imag * gain_imag, real * gain_imag + imag * gain_real],
                    axis=1,
                )
            )
        filtered = jnp.concatenate(parts, axis=0).astype(BF)
        returned = dot(legendre_back[...], filtered).astype(BF)
        send_two_main[...] = returned.reshape(SHT, 4, 2 * HALF)
        exchange(send_two_main, recv_two_main, sent.at[2], got.at[2])

        wait_all(recv_one_rest, got.at[1])
        coeffs = dot(legendre[...], recv_one_rest[...].reshape(2 * NLAT, HALF))
        parts = []
        for order in range(2):
            rest = coeffs[order * LMAX : (order + 1) * LMAX]
            parts.append(rest * gain_straight + pltpu.roll(rest, HALF // 2, 1) * gain_cross)
        filtered = jnp.concatenate(parts, axis=0).astype(BF)
        returned = dot(legendre_back[...], filtered).astype(BF)
        send_two_rest[...] = returned.reshape(SHT, 4, HALF)
        exchange(send_two_rest, recv_two_rest, sent.at[3], got.at[3])

        @pl.when(away)
        def _():
            collect(2, block)
            copy = share(2, block)
            copy.start()
            copy.wait()

        following = jnp.minimum(block + 1, SECTIONS - 1)

        @pl.when(jnp.logical_and(section != following, block < SECTIONS - 1))
        def _():
            hand_out(following)

        @pl.when(jnp.logical_and(section == block + 2, holds))
        def _():
            send_weights(1)
            send_weights(2)

        for turn in (1, 2):

            @pl.when(jnp.logical_and(block == turn, section == 2))
            def _():
                pl.semaphore_signal(
                    pace, inc=1, device_id={"section": turn + 2}, device_id_type=MESH
                )

        skip = matrices[block, :, 0:PAD]
        into = matrices[block, :, PAD : PAD + HID]
        back = matrices[block, :, PAD + HID :]
        for lat in range(2):
            skipped[lat] = dot(normed[lat], skip)

        wait_all(send_one_main, sent.at[0])
        wait_all(send_one_rest, sent.at[1])
        wait_all(recv_two_main, got.at[2])
        wait_all(recv_two_rest, got.at[3])
        slot = lax.rem(block, 2)
        for lat in range(2):
            at = pl.ds(2 * lat, 2)
            waves = recv_two_main[:, at, :].reshape(MMAX, 2 * HALF)
            rest = recv_two_rest[:, at, :].reshape(MMAX, HALF).astype(F32)
            top = jnp.where(low, rest, 0.0).astype(BF)
            bottom = jnp.where(low, pltpu.roll(rest, HALF // 2, 1), 0.0).astype(BF)
            stacked = jnp.concatenate(
                [
                    jnp.concatenate([waves[:, :HALF], top], axis=1),
                    jnp.concatenate([waves[:, HALF:], bottom], axis=1),
                ],
                axis=0,
            )
            activated = gelu(dot(inverse_fourier[...], stacked) + skipped[lat])
            second = layer_norm(activated, gains[block, 1:2, :]).astype(BF)
            hidden = gelu(dot(second, into)).astype(BF)
            update = lax.dot_general(
                hidden, back, (((1,), (1,)), ((), ())), preferred_element_type=F32
            )
            result = state[lat].astype(F32) + update
            state[lat] = result.astype(BF)

            @pl.when(block >= 2)
            def _():
                wait_left(lat, slot)

            odd = pltpu.roll(result[NLON // 2 :, :HALF], HALF // 2, 1)
            odd_rest = pltpu.roll(result[NLON // 2 :, HALF:], HALF // 2, 1)
            leaving[slot, lat] = jnp.concatenate(
                [
                    result[: NLON // 2, :HALF],
                    jnp.where(low, result[: NLON // 2, HALF:], odd),
                    jnp.where(low, odd, odd_rest),
                ],
                axis=1,
            ).astype(BF)

            @pl.when(away)
            def _():
                out_copy(lat, slot, own, block).start()

            @pl.when(jnp.logical_not(away))
            def _():
                own_copy(lat, slot, own).start()

        wait_all(send_two_main, sent.at[2])
        wait_all(send_two_rest, sent.at[3])
        return carry

    @pl.when(holds)
    def _():
        begin[section] = outgoing[own]
        build_legendre(me, rows, lower, upper, first, table, legendre, legendre_back)
        slots = begin.at[pl.ds(0, SECTIONS - 1)]
        pltpu.make_async_copy(slots, slots, member_got).wait()

        @pl.when(section == 1)
        def _():
            send_weights(1)
            send_weights(2)

        for lat in range(2):
            grid = begin[:, lat].astype(F32).reshape(C, NLON).T
            for tile in range(2):
                part = grid[:, :HALF]
                if tile:
                    part = jnp.concatenate(
                        [grid[:, HALF:], jnp.zeros((NLON, PAD - C), F32)], axis=1
                    )
                stage[tile] = part
                for odd in range(2):
                    rows_of = pl.ds(odd * HALF, HALF)
                    state[lat, rows_of, pl.ds(tile * HALF, HALF)] = stage[
                        tile, pl.ds(odd, HALF, stride=2), :
                    ].astype(BF)
        lax.fori_loop(0, SECTIONS, step, 0)
        for slot in range(2):
            for lat in range(2):
                wait_left(lat, slot)

    for target in HOME:

        @pl.when(section != target)
        def _():
            for i in range(3):
                weight_copy(i, target).wait_send()

    for member in range(MEMBERS):

        @pl.when(section != HOME[member])
        def _():
            member_copy(member).wait_send()
            for lat in range(2):
                ref = out.at[member, lat]
                pltpu.make_async_copy(ref, ref, out_got.at[member, lat]).wait()


def per_device(
    analysis, perturbations, gain_first, spectral_gain, skip_weight, gain_second, mlp_in, mlp_out
):
    lats = analysis.shape[0]
    tiles = spectral_gain[0].reshape(2, LMAX // 2, 3, HALF)
    forward, inverse = longitude_tables()
    hbm = pl.BlockSpec(memory_space=pltpu.HBM)
    out = pl.pallas_call(
        kernel,
        out_shape=jax.ShapeDtypeStruct((MEMBERS, lats, NLON // 2, 2 * C), BF),
        in_specs=[hbm] * 11,
        out_specs=hbm,
        scratch_shapes=[
            pltpu.VMEM((lats, C // SECTIONS, NLON), BF),
            pltpu.VMEM((MEMBERS, lats, C // SECTIONS, NLON), BF),
            pltpu.VMEM((1, C), F32),
            pltpu.VMEM((1, C), F32),
            pltpu.VMEM((LMAX // 2, 3, 2, HALF), F32),
            pltpu.VMEM((C, C), BF),
            pltpu.VMEM((2, MMAX, NLON), BF),
            pltpu.VMEM((NLON, 2 * MMAX), BF),
            pltpu.VMEM((8, 2 * NLAT), F32),
            pltpu.SemaphoreType.DMA((11,)),
            pltpu.VMEM((MEMBERS, lats, C // SECTIONS, NLON), BF),
            pltpu.VMEM((SECTIONS, lats, C // SECTIONS, NLON), BF),
            pltpu.VMEM((2, NLON, HALF), F32),
            pltpu.VMEM((2, NLON, PAD), BF),
            pltpu.VMEM((2, NLON, PAD), BF),
            pltpu.VMEM((2, NLON, PAD), F32),
            *[pltpu.VMEM((SHT, 4, 2 * HALF), BF)] * 4,
            *[pltpu.VMEM((SHT, 4, HALF), BF)] * 4,
            pltpu.VMEM((SECTIONS, 8, PAD), F32),
            pltpu.VMEM((SECTIONS, LMAX, 2 * C), BF),
            pltpu.VMEM((SECTIONS, PAD, 1024), BF),
            pltpu.VMEM((LMAX, 2 * NLAT), F32),
            pltpu.VMEM((LMAX, 2 * NLAT), F32),
            pltpu.VMEM((LMAX, 2 * NLAT), F32),
            pltpu.VMEM((LMAX, 2 * NLAT), F32),
            pltpu.VMEM((2 * LMAX, 2 * NLAT), BF),
            pltpu.VMEM((2 * NLAT, 2 * LMAX), BF),
            pltpu.VMEM((2, 2, NLON // 2, 2 * C), BF),
            pltpu.SemaphoreType.DMA((4,)),
            pltpu.SemaphoreType.DMA((4,)),
            pltpu.SemaphoreType.DMA((3, SECTIONS)),
            pltpu.SemaphoreType.DMA((3, SECTIONS)),
            pltpu.SemaphoreType.DMA((3, 4)),
            pltpu.SemaphoreType.DMA((3, SECTIONS)),
            pltpu.SemaphoreType.DMA((3,)),
            pltpu.SemaphoreType.DMA((3, SECTIONS)),
            pltpu.SemaphoreType.DMA((2, 2)),
            pltpu.SemaphoreType.DMA((MEMBERS, 2)),
            pltpu.SemaphoreType.DMA((MEMBERS,)),
            pltpu.SemaphoreType.DMA,
            pltpu.SemaphoreType.REGULAR,
        ],
        compiler_params=pltpu.CompilerParams(
            collective_id=0, has_side_effects=True, vmem_limit_bytes=67_000_000
        ),
    )(
        jnp.transpose(analysis, (0, 2, 1)),
        jnp.transpose(perturbations, (0, 1, 3, 2)),
        gain_first,
        gain_second,
        jnp.transpose(tiles, (1, 2, 0, 3)),
        skip_weight[0],
        mlp_in[0],
        mlp_out[0],
        forward,
        inverse,
        latitude_rows(),
    )
    return out.reshape(1, MEMBERS, lats, NLON * C)


def solution(mesh):
    return jax.shard_map(
        per_device,
        mesh=mesh,
        in_specs=(
            P("sht", None, "section"),
            P(None, "sht", None, "section"),
            P("section", None),
            P("section", None, None),
            P("section", None, None),
            P("section", None),
            P("section", None, None),
            P("section", None, None),
        ),
        out_specs=P("section", None, "sht", None),
        check_vma=False,
    )
```

```python
import math

import jax
import jax.numpy as jnp
import numpy as np
from jax import lax
from jax.experimental import pallas as pl
from jax.experimental.pallas import tpu as pltpu
from jax.sharding import PartitionSpec as P

C = 192
HID = 384
NLAT = 128
NLON = 256
LMAX = 128
MMAX = 128
MEMBERS = 6
SECTIONS = 8
SHT = 64
HOME = (5, 6, 7, 0, 1, 2)
PAD = 256
HALF = 128
MESH = pl.DeviceIdType.MESH
BF = jnp.bfloat16
F32 = jnp.float32


def partner_offsets():
    hops = lambda o: min(o[0], 4 - o[0]) + min(o[1], 8 - o[1])
    offsets = [(dx, dy) for dx in range(4) for dy in range(8)]
    return sorted(offsets, key=lambda o: (-hops(o), o[1] % 2, o[0]))


def partners(chip_x, chip_y, core):
    for dx, dy in partner_offsets():
        base = lax.rem(chip_x + dx, 4) * 16 + lax.rem(chip_y + dy, 8) * 2
        for turn in (0, 1) if dx or dy else (1,):
            yield base + lax.rem(core + turn, 2)


def longitude_tables():
    order = np.concatenate([np.arange(0, NLON, 2), np.arange(1, NLON, 2)])
    waves = np.arange(MMAX)
    phase = (waves[:, None] * order[None, :] % NLON).astype(np.float32) * np.float32(
        2.0 * math.pi / NLON
    )
    cosines = np.cos(phase)
    sines = np.sin(phase)
    forward = np.stack([cosines, -sines])
    factor = np.where(waves == 0, 1.0, 2.0).astype(np.float32)
    inverse = np.concatenate([cosines.T * factor, -sines.T * factor], axis=1)
    return jnp.asarray(forward, BF), jnp.asarray(inverse, BF)


def latitude_rows():
    lane = np.arange(2 * NLAT)
    latitude = 2 * (lane % NLAT // 2) + lane // NLAT
    colatitude = (math.pi * (latitude + 0.5) / NLAT).astype(np.float32)
    sine = np.sin(colatitude)
    rows = np.zeros((8, 2 * NLAT), np.float32)
    rows[0] = np.cos(colatitude)
    rows[1] = sine
    rows[2] = np.log(sine)
    rows[3] = sine * (2.0 * math.pi / NLON) * (math.pi / NLAT)
    rows[4] = lane % 2
    return jnp.asarray(rows)


def gelu(x):
    return 0.5 * x * (1.0 + lax.erf(x * math.sqrt(0.5)))


def lane_of(shape):
    return lax.broadcasted_iota(jnp.int32, shape, len(shape) - 1)


def layer_norm(values, gain_row):
    average = jnp.sum(values, axis=1, keepdims=True) * (1.0 / C)
    centred = jnp.where(lane_of(values.shape) < C, values - average, 0.0)
    variance = jnp.sum(centred * centred, axis=1, keepdims=True) * (1.0 / C)
    return centred * lax.rsqrt(variance + 1e-05) * gain_row


def dot(a, b):
    return jnp.dot(a, b, preferred_element_type=F32)


def build_legendre(me, rows_ref, lower, upper, first, table, forward_table, inverse_table):
    cosine = rows_ref[0:1, :]
    parity = rows_ref[4:5, :]
    order = parity + (2 * me).astype(F32)
    shape = (LMAX, 2 * NLAT)
    degree = lax.broadcasted_iota(jnp.int32, shape, 0).astype(F32)
    step = degree + 1.0
    terms = jnp.where(step <= order, 0.5 * jnp.log((2.0 * step + 1.0) / (2.0 * step)), 0.0)
    picked = jnp.sum(terms, axis=0, keepdims=True)
    diagonal = jnp.exp(picked + order * rows_ref[2:3, :]) * math.sqrt(0.25 / math.pi)
    lower[...] = jnp.sqrt(
        jnp.maximum(4.0 * degree * degree - 1.0, 0.0)
        / jnp.maximum(degree * degree - order * order, 1.0)
    )
    shifted = degree - 1.0
    upper[...] = jnp.sqrt(
        jnp.maximum(shifted * shifted - order * order, 0.0)
        / jnp.maximum(4.0 * shifted * shifted - 1.0, 1.0)
    )
    first[...] = jnp.where(degree == order, diagonal, 0.0)

    def advance(row, carry):
        latest, earlier = carry
        at = pl.ds(row, 1)
        current = lower[at, :] * (cosine * latest - upper[at, :] * earlier) + first[at, :]
        table[pl.ds(lax.rem(row, 2) * (LMAX // 2) + row // 2, 1), :] = current
        return (current, latest)

    zero = cosine * 0.0
    lax.fori_loop(0, LMAX, advance, (zero, zero), unroll=8)
    plain = table[...]
    weighted = plain * rows_ref[3:4, :]
    even = jnp.broadcast_to(parity, shape) < 0.5
    forward_table[0:LMAX, :] = jnp.where(even, weighted, 0.0).astype(BF)
    forward_table[LMAX:, :] = jnp.where(even, 0.0, weighted).astype(BF)
    inverse_table[:, 0:LMAX] = jnp.where(even, plain, 0.0).T.astype(BF)
    inverse_table[:, LMAX:] = jnp.where(even, 0.0, plain).T.astype(BF)


def kernel(
    analysis_in, perturbations_in, gain_first_in, gain_second_in, gain_tiles_in, skip_in,
    mlp_in, mlp_out, fourier_in, inverse_fourier_in, rows_in,
    out,
    analysis, perturbations, gain_first, gain_second, gain_tiles, skip_own,
    fourier, inverse_fourier, rows, loaded,
    outgoing, begin, stage, state, normed, skipped,
    send_one, send_two, recv_one, recv_two,
    gains, filters, matrices, lower, upper, first, table, legendre, legendre_back, leaving,
    sent, got, weight_sent, weight_got, pass_sent, pass_got,
    share_sent, share_got, out_sent, out_got, member_sent, member_got, pace,
):
    section = lax.axis_index("section")
    me = lax.axis_index("sht")
    core = lax.rem(me, 2)
    sibling = me + 1 - 2 * core
    own = lax.rem(section + 3, SECTIONS)
    holds = own < MEMBERS
    chip_x = me // 16
    chip_y = lax.rem(me // 2, 8)

    loads = [
        pltpu.make_async_copy(source, target, loaded.at[i])
        for i, (source, target) in enumerate(
            [
                (perturbations_in, perturbations),
                (analysis_in, analysis),
                (gain_first_in, gain_first),
                (gain_second_in, gain_second),
                (gain_tiles_in, gain_tiles),
                (skip_in, skip_own),
                (mlp_in, matrices.at[section, pl.ds(0, C), pl.ds(PAD, HID)]),
                (mlp_out, matrices.at[section, pl.ds(0, C), pl.ds(PAD + HID, HID)]),
                (rows_in, rows),
                (fourier_in, fourier),
                (inverse_fourier_in, inverse_fourier),
            ]
        )
    ]
    for load in loads:
        load.start()
    barrier = pltpu.get_barrier_semaphore()

    def greet_column(t, carry):
        pl.semaphore_signal(
            barrier, inc=1, device_id={"section": lax.rem(section + t, SECTIONS)},
            device_id_type=MESH,
        )
        return carry

    for to in partners(chip_x, chip_y, core):
        pl.semaphore_signal(barrier, inc=1, device_id={"sht": to}, device_id_type=MESH)
    lax.fori_loop(1, SECTIONS, greet_column, 0)

    loads[0].wait()
    loads[1].wait()
    deviations = perturbations[...].astype(F32)
    average = jnp.sum(deviations, axis=0) * (1.0 / MEMBERS)
    centre = analysis[...].astype(F32)
    for member in range(MEMBERS):
        outgoing[member] = (centre + deviations[member] - average).astype(BF)

    for load in loads[2:8]:
        load.wait()
    gains[section] = jnp.zeros((8, PAD), F32)
    gains[section, 0:1, 0:C] = gain_first[...]
    gains[section, 1:2, 0:C] = gain_second[...]
    tiles = [[gain_tiles[:, third, p, :] for third in range(3)] for p in range(2)]
    turned = [[pltpu.roll(tile, HALF // 2, 1) for tile in row] for row in tiles]
    left = lane_of((LMAX // 2, HALF)) < HALF // 2
    even_rows, odd_rows = pl.ds(0, LMAX // 2), pl.ds(LMAX // 2, LMAX // 2)
    for p in range(2):
        at = pl.ds(p * HALF, HALF)
        filters[section, even_rows, at] = tiles[p][0].astype(BF)
        filters[section, odd_rows, at] = jnp.where(left, turned[p][1], turned[p][2]).astype(BF)
    at = pl.ds(2 * HALF, HALF)
    filters[section, even_rows, at] = jnp.where(left, tiles[0][1], turned[1][1]).astype(BF)
    filters[section, odd_rows, at] = jnp.where(left, turned[0][2], tiles[1][2]).astype(BF)
    matrices[:, C:, :] = jnp.zeros((SECTIONS, PAD - C, 1024), BF)
    matrices[section, 0:C, 0:PAD] = jnp.concatenate(
        [skip_own[...], jnp.zeros((C, PAD - C), BF)], axis=1
    )
    for load in loads[8:]:
        load.wait()

    pl.semaphore_wait(barrier, SHT - 1 + SECTIONS - 1)

    def member_copy(member):
        return pltpu.make_async_remote_copy(
            src_ref=outgoing.at[member], dst_ref=begin.at[section],
            send_sem=member_sent.at[member], recv_sem=member_got,
            device_id={"section": lax.rem(member + 5, SECTIONS)}, device_id_type=MESH,
        )

    for turn in (4, 3, 5, 2, 6, 1, 7):
        member = lax.rem(own + turn, SECTIONS)

        @pl.when(member < MEMBERS)
        def _():
            member_copy(member).start()

    filter_half = pl.ds(pl.multiple_of(core * (LMAX // 2), LMAX // 2), LMAX // 2)
    matrix_half = pl.ds(pl.multiple_of(core * 512, 512), 512)
    filter_piece = pl.ds(pl.multiple_of(core * 64 + chip_x * 16, 16), 16)
    matrix_piece = pl.ds(pl.multiple_of(core * 512 + chip_x * HALF, HALF), HALF)

    def part_of(i, block, piece):
        if i == 0:
            return gains.at[block]
        if i == 1:
            return filters.at[block, filter_piece if piece else filter_half]
        return matrices.at[block, pl.ds(0, C), matrix_piece if piece else matrix_half]

    def weight_copy(i, target):
        ref = part_of(i, section, True)
        return pltpu.make_async_remote_copy(
            src_ref=ref, dst_ref=ref, send_sem=weight_sent.at[i, target],
            recv_sem=weight_got.at[i, section], device_id={"section": target},
            device_id_type=MESH,
        )

    def send_weights(i):
        for target in HOME:

            @pl.when(section != target)
            def _():
                weight_copy(i, target).start()

    def arrived(i, block):
        ref = part_of(i, block, True)
        pltpu.make_async_copy(ref, ref, weight_got.at[i, block]).wait()

    def share(i, block):
        ref = part_of(i, block, False)
        return pltpu.make_async_remote_copy(
            src_ref=ref, dst_ref=ref, send_sem=share_sent.at[i], recv_sem=share_got.at[i, block],
            device_id={"sht": sibling}, device_id_type=MESH,
        )

    def pass_along(i, block, step):
        ref = part_of(i, block, True)
        to = lax.rem(chip_x + step, 4) * 16 + lax.rem(me, 16)
        return pltpu.make_async_remote_copy(
            src_ref=ref, dst_ref=ref, send_sem=pass_sent.at[i, step],
            recv_sem=pass_got.at[i, block], device_id={"sht": to}, device_id_type=MESH,
        )

    def hand_out(block):
        for i in (1, 2):
            arrived(i, block)
            for step in range(1, 4):
                pass_along(i, block, step).start()

    def collect(i, block):
        ref = filters.at[0, pl.ds(0, 48)] if i == 1 else matrices.at[0, pl.ds(0, C), pl.ds(0, 384)]
        pltpu.make_async_copy(ref, ref, pass_got.at[i, block]).wait()
        for step in range(1, 4):
            pass_along(i, block, step).wait_send()

    send_weights(0)

    @pl.when(section == 0)
    def _():
        send_weights(1)
        send_weights(2)

    @pl.when(jnp.logical_not(holds))
    def _():
        pl.semaphore_wait(pace, 1)
        send_weights(1)
        send_weights(2)

    def exchange(send, recv, sent, got):
        recv[me] = send[me]
        for to in partners(chip_x, chip_y, core):
            pltpu.make_async_remote_copy(
                src_ref=send.at[to], dst_ref=recv.at[me], send_sem=sent, recv_sem=got,
                device_id={"sht": to}, device_id_type=MESH,
            ).start()

    def wait_all(buffer, semaphore):
        ref = buffer.at[pl.ds(0, SHT - 1)]
        pltpu.make_async_copy(ref, ref, semaphore).wait()

    def out_copy(lat, slot, member, block):
        return pltpu.make_async_remote_copy(
            src_ref=leaving.at[slot, lat], dst_ref=out.at[member, lat],
            send_sem=out_sent.at[slot, lat], recv_sem=out_got.at[member, lat],
            device_id={"section": block}, device_id_type=MESH,
        )

    def own_copy(lat, slot, member):
        return pltpu.make_async_copy(
            leaving.at[slot, lat], out.at[member, lat], out_sent.at[slot, lat]
        )

    def wait_left(lat, slot):
        ref = leaving.at[slot, lat]
        pltpu.make_async_copy(ref, ref, out_sent.at[slot, lat]).wait()

    low = lane_of((HALF, HALF)) < HALF // 2
    low_all = lane_of((NLON, HALF)) < HALF // 2

    def begin_block(lat, block):
        wide = layer_norm(state[lat].astype(F32), gains[block, 0:1, :])
        narrow = wide.astype(BF)
        normed[lat] = narrow
        turned = pltpu.roll(wide[:, HALF:], HALF // 2, 1).astype(BF)
        real = dot(fourier[0], narrow)
        imag = dot(fourier[1], jnp.concatenate([narrow[:, :HALF], turned], axis=1))
        spectrum = jnp.concatenate(
            [real[:, :HALF], imag[:, :HALF], real[:, HALF:] + imag[:, HALF:]], axis=1
        ).astype(BF)
        send_one[lat] = spectrum.reshape(SHT, 2, 2 * C)
        exchange(send_one.at[lat], recv_one.at[lat], sent.at[lat], got.at[lat])

    def step(block, carry):
        away = section != block

        @pl.when(jnp.logical_and(away, block == 0))
        def _():
            hand_out(0)

        @pl.when(away)
        def _():
            collect(1, block)
            copy = share(1, block)
            copy.start()
            copy.wait()

        gain = filters[block].astype(F32)
        gain_real, gain_imag = gain[:, :HALF], gain[:, HALF : 2 * HALF]
        gain_rest = gain[:, 2 * HALF :]
        gain_turned = pltpu.roll(gain_rest, HALF // 2, 1)
        gain_straight = jnp.where(low, gain_rest, gain_turned)
        gain_cross = jnp.where(low, -gain_turned, gain_rest)

        wait_all(recv_one.at[0], got.at[0])
        coeffs = dot(legendre[:, :NLAT], recv_one[0].reshape(NLAT, 2 * C))
        wait_all(recv_one.at[1], got.at[1])
        coeffs = coeffs + dot(legendre[:, NLAT:], recv_one[1].reshape(NLAT, 2 * C))
        parts = []
        for order in range(2):
            part = coeffs[order * LMAX : (order + 1) * LMAX]
            real, imag, rest = part[:, :HALF], part[:, HALF : 2 * HALF], part[:, 2 * HALF :]
            parts.append(
                jnp.concatenate(
                    [
                        real * gain_real - imag * gain_imag,
                        real * gain_imag + imag * gain_real,
                        rest * gain_straight + pltpu.roll(rest, HALF // 2, 1) * gain_cross,
                    ],
                    axis=1,
                )
            )
        filtered = jnp.concatenate(parts, axis=0).astype(BF)
        for lat in range(2):
            returned = dot(legendre_back[lat * NLAT : (lat + 1) * NLAT, :], filtered).astype(BF)
            send_two[lat] = returned.reshape(SHT, 2, 2 * C)
            exchange(send_two.at[lat], recv_two.at[lat], sent.at[2 + lat], got.at[2 + lat])

        @pl.when(away)
        def _():
            collect(2, block)
            copy = share(2, block)
            copy.start()
            copy.wait()

        following = jnp.minimum(block + 1, SECTIONS - 1)

        @pl.when(jnp.logical_and(section != following, block < SECTIONS - 1))
        def _():
            arrived(0, following)
            hand_out(following)

        @pl.when(jnp.logical_and(section == block + 2, holds))
        def _():
            send_weights(1)
            send_weights(2)

        for turn in (1, 2):

            @pl.when(jnp.logical_and(block == turn, section == 2))
            def _():
                pl.semaphore_signal(
                    pace, inc=1, device_id={"section": turn + 2}, device_id_type=MESH
                )

        skip = matrices[block, :, 0:PAD]
        into = matrices[block, :, PAD : PAD + HID]
        back = matrices[block, :, PAD + HID :]
        for lat in range(2):
            skipped[lat] = dot(normed[lat], skip)

        for lat in range(2):
            wait_all(send_one.at[lat], sent.at[lat])
        slot = lax.rem(block, 2)
        for lat in range(2):
            wait_all(recv_two.at[lat], got.at[2 + lat])
            waves = recv_two[lat].reshape(MMAX, 2 * C)
            rest = waves[:, 2 * HALF :].astype(F32)
            top = jnp.where(low, rest, 0.0).astype(BF)
            bottom = jnp.where(low, pltpu.roll(rest, HALF // 2, 1), 0.0).astype(BF)
            stacked = jnp.concatenate(
                [
                    jnp.concatenate([waves[:, :HALF], top], axis=1),
                    jnp.concatenate([waves[:, HALF : 2 * HALF], bottom], axis=1),
                ],
                axis=0,
            )
            activated = gelu(dot(inverse_fourier[...], stacked) + skipped[lat])
            second = layer_norm(activated, gains[block, 1:2, :]).astype(BF)
            hidden = gelu(dot(second, into)).astype(BF)
            update = lax.dot_general(
                hidden, back, (((1,), (1,)), ((), ())), preferred_element_type=F32
            )
            result = state[lat].astype(F32) + update
            state[lat] = result.astype(BF)

            @pl.when(block < SECTIONS - 1)
            def _():
                begin_block(lat, following)

            @pl.when(block >= 2)
            def _():
                wait_left(lat, slot)

            odd = pltpu.roll(result[NLON // 2 :, :HALF], HALF // 2, 1)
            odd_rest = pltpu.roll(result[NLON // 2 :, HALF:], HALF // 2, 1)
            leaving[slot, lat] = jnp.concatenate(
                [
                    result[: NLON // 2, :HALF],
                    jnp.where(low, result[: NLON // 2, HALF:], odd),
                    jnp.where(low, odd, odd_rest),
                ],
                axis=1,
            ).astype(BF)

            @pl.when(away)
            def _():
                out_copy(lat, slot, own, block).start()

            @pl.when(jnp.logical_not(away))
            def _():
                own_copy(lat, slot, own).start()

        for lat in range(2):
            wait_all(send_two.at[lat], sent.at[2 + lat])
        return carry

    @pl.when(holds)
    def _():
        begin[section] = outgoing[own]
        build_legendre(me, rows, lower, upper, first, table, legendre, legendre_back)
        slots = begin.at[pl.ds(0, SECTIONS - 1)]
        pltpu.make_async_copy(slots, slots, member_got).wait()

        @pl.when(section == 1)
        def _():
            send_weights(1)
            send_weights(2)

        for lat in range(2):
            grid = begin[:, lat].astype(F32).reshape(C, NLON).T
            for tile in range(2):
                part = grid[:, :HALF]
                if tile:
                    part = jnp.concatenate(
                        [grid[:, HALF:], jnp.zeros((NLON, PAD - C), F32)], axis=1
                    )
                stage[tile] = part
                for odd in range(2):
                    rows_of = pl.ds(odd * HALF, HALF)
                    state[lat, rows_of, pl.ds(tile * HALF, HALF)] = stage[
                        tile, pl.ds(odd, HALF, stride=2), :
                    ].astype(BF)

        @pl.when(section != 0)
        def _():
            arrived(0, 0)

        for lat in range(2):
            begin_block(lat, 0)
        lax.fori_loop(0, SECTIONS, step, 0)
        for slot in range(2):
            for lat in range(2):
                wait_left(lat, slot)

    for target in HOME:

        @pl.when(section != target)
        def _():
            for i in range(3):
                weight_copy(i, target).wait_send()

    for member in range(MEMBERS):

        @pl.when(section != HOME[member])
        def _():
            member_copy(member).wait_send()
            for lat in range(2):
                ref = out.at[member, lat]
                pltpu.make_async_copy(ref, ref, out_got.at[member, lat]).wait()


def per_device(
    analysis, perturbations, gain_first, spectral_gain, skip_weight, gain_second, mlp_in, mlp_out
):
    lats = analysis.shape[0]
    tiles = spectral_gain[0].reshape(2, LMAX // 2, 3, HALF)
    forward, inverse = longitude_tables()
    hbm = pl.BlockSpec(memory_space=pltpu.HBM)
    out = pl.pallas_call(
        kernel,
        out_shape=jax.ShapeDtypeStruct((MEMBERS, lats, NLON // 2, 2 * C), BF),
        in_specs=[hbm] * 11,
        out_specs=hbm,
        scratch_shapes=[
            pltpu.VMEM((lats, C // SECTIONS, NLON), BF),
            pltpu.VMEM((MEMBERS, lats, C // SECTIONS, NLON), BF),
            pltpu.VMEM((1, C), F32),
            pltpu.VMEM((1, C), F32),
            pltpu.VMEM((LMAX // 2, 3, 2, HALF), F32),
            pltpu.VMEM((C, C), BF),
            pltpu.VMEM((2, MMAX, NLON), BF),
            pltpu.VMEM((NLON, 2 * MMAX), BF),
            pltpu.VMEM((8, 2 * NLAT), F32),
            pltpu.SemaphoreType.DMA((11,)),
            pltpu.VMEM((MEMBERS, lats, C // SECTIONS, NLON), BF),
            pltpu.VMEM((SECTIONS, lats, C // SECTIONS, NLON), BF),
            pltpu.VMEM((2, NLON, HALF), F32),
            pltpu.VMEM((2, NLON, PAD), BF),
            pltpu.VMEM((2, NLON, PAD), BF),
            pltpu.VMEM((2, NLON, PAD), F32),
            *[pltpu.VMEM((lats, SHT, 2, 2 * C), BF)] * 4,
            pltpu.VMEM((SECTIONS, 8, PAD), F32),
            pltpu.VMEM((SECTIONS, LMAX, 2 * C), BF),
            pltpu.VMEM((SECTIONS, PAD, 1024), BF),
            pltpu.VMEM((LMAX, 2 * NLAT), F32),
            pltpu.VMEM((LMAX, 2 * NLAT), F32),
            pltpu.VMEM((LMAX, 2 * NLAT), F32),
            pltpu.VMEM((LMAX, 2 * NLAT), F32),
            pltpu.VMEM((2 * LMAX, 2 * NLAT), BF),
            pltpu.VMEM((2 * NLAT, 2 * LMAX), BF),
            pltpu.VMEM((2, 2, NLON // 2, 2 * C), BF),
            pltpu.SemaphoreType.DMA((4,)),
            pltpu.SemaphoreType.DMA((4,)),
            pltpu.SemaphoreType.DMA((3, SECTIONS)),
            pltpu.SemaphoreType.DMA((3, SECTIONS)),
            pltpu.SemaphoreType.DMA((3, 4)),
            pltpu.SemaphoreType.DMA((3, SECTIONS)),
            pltpu.SemaphoreType.DMA((3,)),
            pltpu.SemaphoreType.DMA((3, SECTIONS)),
            pltpu.SemaphoreType.DMA((2, 2)),
            pltpu.SemaphoreType.DMA((MEMBERS, 2)),
            pltpu.SemaphoreType.DMA((MEMBERS,)),
            pltpu.SemaphoreType.DMA,
            pltpu.SemaphoreType.REGULAR,
        ],
        compiler_params=pltpu.CompilerParams(
            collective_id=0, has_side_effects=True, vmem_limit_bytes=67_000_000
        ),
    )(
        jnp.transpose(analysis, (0, 2, 1)),
        jnp.transpose(perturbations, (0, 1, 3, 2)),
        gain_first,
        gain_second,
        jnp.transpose(tiles, (1, 2, 0, 3)),
        skip_weight[0],
        mlp_in[0],
        mlp_out[0],
        forward,
        inverse,
        latitude_rows(),
    )
    return out.reshape(1, MEMBERS, lats, NLON * C)


def solution(mesh):
    return jax.shard_map(
        per_device,
        mesh=mesh,
        in_specs=(
            P("sht", None, "section"),
            P(None, "sht", None, "section"),
            P("section", None),
            P("section", None, None),
            P("section", None, None),
            P("section", None),
            P("section", None, None),
            P("section", None, None),
        ),
        out_specs=P("section", None, "sht", None),
        check_vma=False,
    )
```

```python
import math

import jax
import jax.numpy as jnp
import numpy as np
from jax import lax
from jax.experimental import pallas as pl
from jax.experimental.pallas import tpu as pltpu
from jax.sharding import PartitionSpec as P

C = 192
HID = 384
NLAT = 128
NLON = 256
LMAX = 128
MMAX = 128
MEMBERS = 6
SECTIONS = 8
SHT = 64
HOME = (5, 6, 7, 0, 1, 2)
PAD = 256
FAR = 32
HALF = 128
MESH = pl.DeviceIdType.MESH
BF = jnp.bfloat16
F32 = jnp.float32


def partner_offsets():
    hops = lambda o: min(o[0], 4 - o[0]) + min(o[1], 8 - o[1])
    offsets = [(dx, dy) for dx in range(4) for dy in range(8)]
    return sorted(offsets, key=lambda o: (-hops(o), o[1] % 2, o[0]))


def partners(chip_x, chip_y, core):
    for dx, dy in partner_offsets():
        base = lax.rem(chip_x + dx, 4) * 16 + lax.rem(chip_y + dy, 8) * 2
        for turn in (0, 1) if dx or dy else (1,):
            yield base + lax.rem(core + turn, 2)


def longitude_tables():
    order = np.concatenate([np.arange(0, NLON, 2), np.arange(1, NLON, 2)])
    waves = np.arange(MMAX)
    phase = (waves[:, None] * order[None, :] % NLON).astype(np.float32) * np.float32(
        2.0 * math.pi / NLON
    )
    cosines = np.cos(phase)
    sines = np.sin(phase)
    forward = np.stack([cosines, -sines])
    factor = np.where(waves == 0, 1.0, 2.0).astype(np.float32)
    inverse = np.concatenate([cosines.T * factor, -sines.T * factor], axis=1)
    return jnp.asarray(forward, BF), jnp.asarray(inverse, BF)


def latitude_rows():
    lane = np.arange(2 * NLAT)
    latitude = 2 * (lane % NLAT // 2) + lane // NLAT
    colatitude = (math.pi * (latitude + 0.5) / NLAT).astype(np.float32)
    sine = np.sin(colatitude)
    rows = np.zeros((8, 2 * NLAT), np.float32)
    rows[0] = np.cos(colatitude)
    rows[1] = sine
    rows[2] = np.log(sine)
    rows[3] = sine * (2.0 * math.pi / NLON) * (math.pi / NLAT)
    rows[4] = lane % 2
    return jnp.asarray(rows)


def gelu(x):
    return 0.5 * x * (1.0 + lax.erf(x * math.sqrt(0.5)))


def lane_of(shape):
    return lax.broadcasted_iota(jnp.int32, shape, len(shape) - 1)


def layer_norm(values, gain_row):
    average = jnp.sum(values, axis=1, keepdims=True) * (1.0 / C)
    centred = jnp.where(lane_of(values.shape) < C, values - average, 0.0)
    variance = jnp.sum(centred * centred, axis=1, keepdims=True) * (1.0 / C)
    return centred * lax.rsqrt(variance + 1e-05) * gain_row


def dot(a, b):
    return jnp.dot(a, b, preferred_element_type=F32)


def build_legendre(me, rows_ref, lower, upper, first, table, forward_table, inverse_table):
    cosine = rows_ref[0:1, :]
    parity = rows_ref[4:5, :]
    order = parity + (2 * me).astype(F32)
    shape = (LMAX, 2 * NLAT)
    degree = lax.broadcasted_iota(jnp.int32, shape, 0).astype(F32)
    step = degree + 1.0
    terms = jnp.where(step <= order, 0.5 * jnp.log((2.0 * step + 1.0) / (2.0 * step)), 0.0)
    picked = jnp.sum(terms, axis=0, keepdims=True)
    diagonal = jnp.exp(picked + order * rows_ref[2:3, :]) * math.sqrt(0.25 / math.pi)
    lower[...] = jnp.sqrt(
        jnp.maximum(4.0 * degree * degree - 1.0, 0.0)
        / jnp.maximum(degree * degree - order * order, 1.0)
    )
    shifted = degree - 1.0
    upper[...] = jnp.sqrt(
        jnp.maximum(shifted * shifted - order * order, 0.0)
        / jnp.maximum(4.0 * shifted * shifted - 1.0, 1.0)
    )
    first[...] = jnp.where(degree == order, diagonal, 0.0)

    def advance(row, carry):
        latest, earlier = carry
        at = pl.ds(row, 1)
        current = lower[at, :] * (cosine * latest - upper[at, :] * earlier) + first[at, :]
        table[pl.ds(lax.rem(row, 2) * (LMAX // 2) + row // 2, 1), :] = current
        return (current, latest)

    zero = cosine * 0.0
    lax.fori_loop(0, LMAX, advance, (zero, zero), unroll=8)
    plain = table[...]
    weighted = plain * rows_ref[3:4, :]
    even = jnp.broadcast_to(parity, shape) < 0.5
    forward_table[0:LMAX, :] = jnp.where(even, weighted, 0.0).astype(BF)
    forward_table[LMAX:, :] = jnp.where(even, 0.0, weighted).astype(BF)
    inverse_table[:, 0:LMAX] = jnp.where(even, plain, 0.0).T.astype(BF)
    inverse_table[:, LMAX:] = jnp.where(even, 0.0, plain).T.astype(BF)


def kernel(
    analysis_in, perturbations_in, gain_first_in, gain_second_in, gain_tiles_in, skip_in,
    mlp_in, mlp_out, fourier_in, inverse_fourier_in, rows_in,
    out,
    analysis, perturbations, gain_first, gain_second, gain_tiles, skip_own,
    fourier, inverse_fourier, rows, loaded, relay, relay_sent, relay_got,
    outgoing, begin, stage, state, normed, skipped,
    send_one, send_two, recv_one, recv_two,
    gains, filters, matrices, lower, upper, first, table, legendre, legendre_back, leaving,
    sent, got, weight_sent, weight_got, pass_sent, pass_got,
    share_sent, share_got, out_sent, out_got, member_sent, member_got, pace,
):
    section = lax.axis_index("section")
    me = lax.axis_index("sht")
    core = lax.rem(me, 2)
    sibling = me + 1 - 2 * core
    own = lax.rem(section + 3, SECTIONS)
    holds = own < MEMBERS
    chip_x = me // 16
    chip_y = lax.rem(me // 2, 8)

    loads = [
        pltpu.make_async_copy(source, target, loaded.at[i])
        for i, (source, target) in enumerate(
            [
                (perturbations_in, perturbations),
                (analysis_in, analysis),
                (gain_first_in, gain_first),
                (gain_second_in, gain_second),
                (gain_tiles_in, gain_tiles),
                (skip_in, skip_own),
                (mlp_in, matrices.at[section, pl.ds(0, C), pl.ds(PAD, HID)]),
                (mlp_out, matrices.at[section, pl.ds(0, C), pl.ds(PAD + HID, HID)]),
                (rows_in, rows),
                (fourier_in, fourier),
                (inverse_fourier_in, inverse_fourier),
            ]
        )
    ]
    for load in loads:
        load.start()
    barrier = pltpu.get_barrier_semaphore()

    def greet_column(t, carry):
        pl.semaphore_signal(
            barrier, inc=1, device_id={"section": lax.rem(section + t, SECTIONS)},
            device_id_type=MESH,
        )
        return carry

    for to in partners(chip_x, chip_y, core):
        pl.semaphore_signal(barrier, inc=1, device_id={"sht": to}, device_id_type=MESH)
    lax.fori_loop(1, SECTIONS, greet_column, 0)

    loads[0].wait()
    loads[1].wait()
    deviations = perturbations[...].astype(F32)
    average = jnp.sum(deviations, axis=0) * (1.0 / MEMBERS)
    centre = analysis[...].astype(F32)
    for member in range(MEMBERS):
        outgoing[member] = (centre + deviations[member] - average).astype(BF)

    for load in loads[2:8]:
        load.wait()
    gains[section] = jnp.zeros((8, PAD), F32)
    gains[section, 0:1, 0:C] = gain_first[...]
    gains[section, 1:2, 0:C] = gain_second[...]
    tiles = [[gain_tiles[:, third, p, :] for third in range(3)] for p in range(2)]
    turned = [[pltpu.roll(tile, HALF // 2, 1) for tile in row] for row in tiles]
    left = lane_of((LMAX // 2, HALF)) < HALF // 2
    even_rows, odd_rows = pl.ds(0, LMAX // 2), pl.ds(LMAX // 2, LMAX // 2)
    for p in range(2):
        at = pl.ds(p * HALF, HALF)
        filters[section, even_rows, at] = tiles[p][0].astype(BF)
        filters[section, odd_rows, at] = jnp.where(left, turned[p][1], turned[p][2]).astype(BF)
    at = pl.ds(2 * HALF, HALF)
    filters[section, even_rows, at] = jnp.where(left, tiles[0][1], turned[1][1]).astype(BF)
    filters[section, odd_rows, at] = jnp.where(left, turned[0][2], tiles[1][2]).astype(BF)
    matrices[:, C:, :] = jnp.zeros((SECTIONS, PAD - C, 1024), BF)
    matrices[section, 0:C, 0:PAD] = jnp.concatenate(
        [skip_own[...], jnp.zeros((C, PAD - C), BF)], axis=1
    )
    for load in loads[8:]:
        load.wait()

    pl.semaphore_wait(barrier, SHT - 1 + SECTIONS - 1)

    def member_copy(member):
        return pltpu.make_async_remote_copy(
            src_ref=outgoing.at[member], dst_ref=begin.at[section],
            send_sem=member_sent.at[member], recv_sem=member_got,
            device_id={"section": lax.rem(member + 5, SECTIONS)}, device_id_type=MESH,
        )

    for turn in (4, 3, 5, 2, 6, 1, 7):
        member = lax.rem(own + turn, SECTIONS)

        @pl.when(member < MEMBERS)
        def _():
            member_copy(member).start()

    filter_half = pl.ds(pl.multiple_of(core * (LMAX // 2), LMAX // 2), LMAX // 2)
    matrix_half = pl.ds(pl.multiple_of(core * 512, 512), 512)
    filter_piece = pl.ds(pl.multiple_of(core * 64 + chip_x * 16, 16), 16)
    matrix_piece = pl.ds(pl.multiple_of(core * 512 + chip_x * HALF, HALF), HALF)

    def part_of(i, block, piece):
        if i == 0:
            return gains.at[block]
        if i == 1:
            return filters.at[block, filter_piece if piece else filter_half]
        return matrices.at[block, pl.ds(0, C), matrix_piece if piece else matrix_half]

    def weight_copy(i, target):
        ref = part_of(i, section, True)
        return pltpu.make_async_remote_copy(
            src_ref=ref, dst_ref=ref, send_sem=weight_sent.at[i, target],
            recv_sem=weight_got.at[i, section], device_id={"section": target},
            device_id_type=MESH,
        )

    def send_weights(i):
        for target in HOME:

            @pl.when(section != target)
            def _():
                weight_copy(i, target).start()

    def arrived(i, block):
        ref = part_of(i, block, True)
        pltpu.make_async_copy(ref, ref, weight_got.at[i, block]).wait()

    def share(i, block):
        ref = part_of(i, block, False)
        return pltpu.make_async_remote_copy(
            src_ref=ref, dst_ref=ref, send_sem=share_sent.at[i], recv_sem=share_got.at[i, block],
            device_id={"sht": sibling}, device_id_type=MESH,
        )

    def pass_along(i, block, step):
        ref = part_of(i, block, True)
        to = lax.rem(chip_x + step, 4) * 16 + lax.rem(me, 16)
        return pltpu.make_async_remote_copy(
            src_ref=ref, dst_ref=ref, send_sem=pass_sent.at[i, step],
            recv_sem=pass_got.at[i, block], device_id={"sht": to}, device_id_type=MESH,
        )

    def hand_out(block):
        for i in (1, 2):
            arrived(i, block)
            for step in range(1, 4):
                pass_along(i, block, step).start()

    def collect(i, block):
        ref = filters.at[0, pl.ds(0, 48)] if i == 1 else matrices.at[0, pl.ds(0, C), pl.ds(0, 384)]
        pltpu.make_async_copy(ref, ref, pass_got.at[i, block]).wait()
        for step in range(1, 4):
            pass_along(i, block, step).wait_send()

    send_weights(0)

    @pl.when(section == 0)
    def _():
        send_weights(1)
        send_weights(2)

    @pl.when(jnp.logical_not(holds))
    def _():
        pl.semaphore_wait(pace, 1)
        send_weights(1)
        send_weights(2)

    def exchange(send, recv, sent, got, first=0, last=SHT - 1):
        if first == 0:
            recv[me] = send[me]
        for to in list(partners(chip_x, chip_y, core))[first:last]:
            pltpu.make_async_remote_copy(
                src_ref=send.at[to], dst_ref=recv.at[me], send_sem=sent, recv_sem=got,
                device_id={"sht": to}, device_id_type=MESH,
            ).start()

    def wait_all(buffer, semaphore):
        ref = buffer.at[pl.ds(0, SHT - 1)]
        pltpu.make_async_copy(ref, ref, semaphore).wait()

    def out_copy(lat, slot, member, block):
        return pltpu.make_async_remote_copy(
            src_ref=leaving.at[slot, lat], dst_ref=out.at[member, lat],
            send_sem=out_sent.at[slot, lat], recv_sem=out_got.at[member, lat],
            device_id={"section": block}, device_id_type=MESH,
        )

    def to_relay():
        return pltpu.make_async_remote_copy(
            src_ref=leaving.at[1, 0], dst_ref=relay, send_sem=out_sent.at[1, 0],
            recv_sem=relay_got, device_id={"section": 4}, device_id_type=MESH,
        )

    def from_relay():
        return pltpu.make_async_remote_copy(
            src_ref=relay, dst_ref=out.at[5, 0], send_sem=relay_sent,
            recv_sem=out_got.at[5, 0], device_id={"section": 7}, device_id_type=MESH,
        )

    def own_copy(lat, slot, member):
        return pltpu.make_async_copy(
            leaving.at[slot, lat], out.at[member, lat], out_sent.at[slot, lat]
        )

    def wait_left(lat, slot):
        ref = leaving.at[slot, lat]
        pltpu.make_async_copy(ref, ref, out_sent.at[slot, lat]).wait()

    low = lane_of((HALF, HALF)) < HALF // 2
    low_all = lane_of((NLON, HALF)) < HALF // 2

    def begin_block(lat, block):
        wide = layer_norm(state[lat].astype(F32), gains[block, 0:1, :])
        narrow = wide.astype(BF)
        normed[lat] = narrow
        turned = pltpu.roll(wide[:, HALF:], HALF // 2, 1).astype(BF)
        real = dot(fourier[0], narrow)
        imag = dot(fourier[1], jnp.concatenate([narrow[:, :HALF], turned], axis=1))
        spectrum = jnp.concatenate(
            [real[:, :HALF], imag[:, :HALF], real[:, HALF:] + imag[:, HALF:]], axis=1
        ).astype(BF)
        send_one[lat] = spectrum.reshape(SHT, 2, 2 * C)
        exchange(send_one.at[lat], recv_one.at[lat], sent.at[lat], got.at[lat], 0, FAR)
        if lat == 1:
            for each in range(2):
                exchange(
                    send_one.at[each], recv_one.at[each], sent.at[each], got.at[each], FAR
                )

    def step(block, carry):
        away = section != block

        @pl.when(jnp.logical_and(away, block == 0))
        def _():
            hand_out(0)

        @pl.when(away)
        def _():
            collect(1, block)
            copy = share(1, block)
            copy.start()
            copy.wait()

        gain = filters[block].astype(F32)
        gain_real, gain_imag = gain[:, :HALF], gain[:, HALF : 2 * HALF]
        gain_rest = gain[:, 2 * HALF :]
        gain_turned = pltpu.roll(gain_rest, HALF // 2, 1)
        gain_straight = jnp.where(low, gain_rest, gain_turned)
        gain_cross = jnp.where(low, -gain_turned, gain_rest)

        wait_all(recv_one.at[0], got.at[0])
        coeffs = dot(legendre[:, :NLAT], recv_one[0].reshape(NLAT, 2 * C))
        wait_all(recv_one.at[1], got.at[1])
        coeffs = coeffs + dot(legendre[:, NLAT:], recv_one[1].reshape(NLAT, 2 * C))
        parts = []
        for order in range(2):
            part = coeffs[order * LMAX : (order + 1) * LMAX]
            real, imag, rest = part[:, :HALF], part[:, HALF : 2 * HALF], part[:, 2 * HALF :]
            parts.append(
                jnp.concatenate(
                    [
                        real * gain_real - imag * gain_imag,
                        real * gain_imag + imag * gain_real,
                        rest * gain_straight + pltpu.roll(rest, HALF // 2, 1) * gain_cross,
                    ],
                    axis=1,
                )
            )
        filtered = jnp.concatenate(parts, axis=0).astype(BF)
        for lat in range(2):
            returned = dot(legendre_back[lat * NLAT : (lat + 1) * NLAT, :], filtered).astype(BF)
            send_two[lat] = returned.reshape(SHT, 2, 2 * C)
            exchange(send_two.at[lat], recv_two.at[lat], sent.at[2 + lat], got.at[2 + lat])

        @pl.when(away)
        def _():
            collect(2, block)
            copy = share(2, block)
            copy.start()
            copy.wait()

        following = jnp.minimum(block + 1, SECTIONS - 1)

        @pl.when(jnp.logical_and(section != following, block < SECTIONS - 1))
        def _():
            arrived(0, following)
            hand_out(following)

        @pl.when(jnp.logical_and(section == block + 2, holds))
        def _():
            send_weights(1)
            send_weights(2)

        for turn in (1, 2):

            @pl.when(jnp.logical_and(block == turn, section == 2))
            def _():
                pl.semaphore_signal(
                    pace, inc=1, device_id={"section": turn + 2}, device_id_type=MESH
                )

        skip = matrices[block, :, 0:PAD]
        into = matrices[block, :, PAD : PAD + HID]
        back = matrices[block, :, PAD + HID :]
        for lat in range(2):
            skipped[lat] = dot(normed[lat], skip)

        for lat in range(2):
            wait_all(send_one.at[lat], sent.at[lat])
        slot = lax.rem(block, 2)
        for lat in range(2):
            wait_all(recv_two.at[lat], got.at[2 + lat])
            waves = recv_two[lat].reshape(MMAX, 2 * C)
            rest = waves[:, 2 * HALF :].astype(F32)
            top = jnp.where(low, rest, 0.0).astype(BF)
            bottom = jnp.where(low, pltpu.roll(rest, HALF // 2, 1), 0.0).astype(BF)
            stacked = jnp.concatenate(
                [
                    jnp.concatenate([waves[:, :HALF], top], axis=1),
                    jnp.concatenate([waves[:, HALF : 2 * HALF], bottom], axis=1),
                ],
                axis=0,
            )
            activated = gelu(dot(inverse_fourier[...], stacked) + skipped[lat])
            second = layer_norm(activated, gains[block, 1:2, :]).astype(BF)
            hidden = gelu(dot(second, into)).astype(BF)
            update = lax.dot_general(
                hidden, back, (((1,), (1,)), ((), ())), preferred_element_type=F32
            )
            result = state[lat].astype(F32) + update
            state[lat] = result.astype(BF)

            @pl.when(block < SECTIONS - 1)
            def _():
                begin_block(lat, following)

            @pl.when(block >= 2)
            def _():
                wait_left(lat, slot)

            odd = pltpu.roll(result[NLON // 2 :, :HALF], HALF // 2, 1)
            odd_rest = pltpu.roll(result[NLON // 2 :, HALF:], HALF // 2, 1)
            leaving[slot, lat] = jnp.concatenate(
                [
                    result[: NLON // 2, :HALF],
                    jnp.where(low, result[: NLON // 2, HALF:], odd),
                    jnp.where(low, odd, odd_rest),
                ],
                axis=1,
            ).astype(BF)

            detour = jnp.logical_and(block == SECTIONS - 1, section == 2)
            if lat == 1:
                detour = False

            @pl.when(jnp.logical_and(away, jnp.logical_not(detour)))
            def _():
                out_copy(lat, slot, own, block).start()

            if lat == 0:

                @pl.when(detour)
                def _():
                    to_relay().start()

            @pl.when(jnp.logical_not(away))
            def _():
                own_copy(lat, slot, own).start()

        for lat in range(2):
            wait_all(send_two.at[lat], sent.at[2 + lat])
        return carry

    @pl.when(holds)
    def _():
        begin[section] = outgoing[own]
        build_legendre(me, rows, lower, upper, first, table, legendre, legendre_back)
        slots = begin.at[pl.ds(0, SECTIONS - 1)]
        pltpu.make_async_copy(slots, slots, member_got).wait()

        @pl.when(section == 1)
        def _():
            send_weights(1)
            send_weights(2)

        for lat in range(2):
            grid = begin[:, lat].astype(F32).reshape(C, NLON).T
            for tile in range(2):
                part = grid[:, :HALF]
                if tile:
                    part = jnp.concatenate(
                        [grid[:, HALF:], jnp.zeros((NLON, PAD - C), F32)], axis=1
                    )
                stage[tile] = part
                for odd in range(2):
                    rows_of = pl.ds(odd * HALF, HALF)
                    state[lat, rows_of, pl.ds(tile * HALF, HALF)] = stage[
                        tile, pl.ds(odd, HALF, stride=2), :
                    ].astype(BF)

        @pl.when(section != 0)
        def _():
            arrived(0, 0)

        for lat in range(2):
            begin_block(lat, 0)
        lax.fori_loop(0, SECTIONS, step, 0)
        for slot in range(2):
            for lat in range(2):
                wait_left(lat, slot)

    @pl.when(section == 4)
    def _():
        pltpu.make_async_copy(relay, relay, relay_got).wait()
        copy = from_relay()
        copy.start()
        copy.wait_send()

    for target in HOME:

        @pl.when(section != target)
        def _():
            for i in range(3):
                weight_copy(i, target).wait_send()

    for member in range(MEMBERS):

        @pl.when(section != HOME[member])
        def _():
            member_copy(member).wait_send()
            for lat in range(2):
                ref = out.at[member, lat]
                pltpu.make_async_copy(ref, ref, out_got.at[member, lat]).wait()


def per_device(
    analysis, perturbations, gain_first, spectral_gain, skip_weight, gain_second, mlp_in, mlp_out
):
    lats = analysis.shape[0]
    tiles = spectral_gain[0].reshape(2, LMAX // 2, 3, HALF)
    forward, inverse = longitude_tables()
    hbm = pl.BlockSpec(memory_space=pltpu.HBM)
    out = pl.pallas_call(
        kernel,
        out_shape=jax.ShapeDtypeStruct((MEMBERS, lats, NLON // 2, 2 * C), BF),
        in_specs=[hbm] * 11,
        out_specs=hbm,
        scratch_shapes=[
            pltpu.VMEM((lats, C // SECTIONS, NLON), BF),
            pltpu.VMEM((MEMBERS, lats, C // SECTIONS, NLON), BF),
            pltpu.VMEM((1, C), F32),
            pltpu.VMEM((1, C), F32),
            pltpu.VMEM((LMAX // 2, 3, 2, HALF), F32),
            pltpu.VMEM((C, C), BF),
            pltpu.VMEM((2, MMAX, NLON), BF),
            pltpu.VMEM((NLON, 2 * MMAX), BF),
            pltpu.VMEM((8, 2 * NLAT), F32),
            pltpu.SemaphoreType.DMA((11,)),
            pltpu.VMEM((NLON // 2, 2 * C), BF),
            pltpu.SemaphoreType.DMA,
            pltpu.SemaphoreType.DMA,
            pltpu.VMEM((MEMBERS, lats, C // SECTIONS, NLON), BF),
            pltpu.VMEM((SECTIONS, lats, C // SECTIONS, NLON), BF),
            pltpu.VMEM((2, NLON, HALF), F32),
            pltpu.VMEM((2, NLON, PAD), BF),
            pltpu.VMEM((2, NLON, PAD), BF),
            pltpu.VMEM((2, NLON, PAD), F32),
            *[pltpu.VMEM((lats, SHT, 2, 2 * C), BF)] * 4,
            pltpu.VMEM((SECTIONS, 8, PAD), F32),
            pltpu.VMEM((SECTIONS, LMAX, 2 * C), BF),
            pltpu.VMEM((SECTIONS, PAD, 1024), BF),
            pltpu.VMEM((LMAX, 2 * NLAT), F32),
            pltpu.VMEM((LMAX, 2 * NLAT), F32),
            pltpu.VMEM((LMAX, 2 * NLAT), F32),
            pltpu.VMEM((LMAX, 2 * NLAT), F32),
            pltpu.VMEM((2 * LMAX, 2 * NLAT), BF),
            pltpu.VMEM((2 * NLAT, 2 * LMAX), BF),
            pltpu.VMEM((2, 2, NLON // 2, 2 * C), BF),
            pltpu.SemaphoreType.DMA((4,)),
            pltpu.SemaphoreType.DMA((4,)),
            pltpu.SemaphoreType.DMA((3, SECTIONS)),
            pltpu.SemaphoreType.DMA((3, SECTIONS)),
            pltpu.SemaphoreType.DMA((3, 4)),
            pltpu.SemaphoreType.DMA((3, SECTIONS)),
            pltpu.SemaphoreType.DMA((3,)),
            pltpu.SemaphoreType.DMA((3, SECTIONS)),
            pltpu.SemaphoreType.DMA((2, 2)),
            pltpu.SemaphoreType.DMA((MEMBERS, 2)),
            pltpu.SemaphoreType.DMA((MEMBERS,)),
            pltpu.SemaphoreType.DMA,
            pltpu.SemaphoreType.REGULAR,
        ],
        compiler_params=pltpu.CompilerParams(
            collective_id=0, has_side_effects=True, vmem_limit_bytes=67_000_000
        ),
    )(
        jnp.transpose(analysis, (0, 2, 1)),
        jnp.transpose(perturbations, (0, 1, 3, 2)),
        gain_first,
        gain_second,
        jnp.transpose(tiles, (1, 2, 0, 3)),
        skip_weight[0],
        mlp_in[0],
        mlp_out[0],
        forward,
        inverse,
        latitude_rows(),
    )
    return out.reshape(1, MEMBERS, lats, NLON * C)


def solution(mesh):
    return jax.shard_map(
        per_device,
        mesh=mesh,
        in_specs=(
            P("sht", None, "section"),
            P(None, "sht", None, "section"),
            P("section", None),
            P("section", None, None),
            P("section", None, None),
            P("section", None),
            P("section", None, None),
            P("section", None, None),
        ),
        out_specs=P("section", None, "sht", None),
        check_vma=False,
    )
```
